128 devices in a mesh: gx: 8 (over x, z_hi), gy: 4 (over y), gz: 4 (over z_lo, core).
Axes of the slice: x: 4, y: 4, z: 4 (z_hi: 2, z_lo: 2; z = z_hi * 2 + z_lo), core: 2. Of those that a mesh axis runs over, the one named last changes fastest.
Arguments:
- point_xyz: float32 [6144, 3, 128], P(('gx', 'gy', 'gz')), may hold values from 0 to 64, as said below
- point_weight: float32 [6144, 128], P(('gx', 'gy', 'gz')), may hold values from 0.25 to 2
- block_cell: int32 [6144], P(('gx', 'gy', 'gz')), may hold values from 0 to 8191, as said below
- block_count: int32 [6144], P(('gx', 'gy', 'gz')), may hold values from 1 to 128, as said below
- gauss_mean: float32 [8, 16, 64, 3, 32], P('gx', 'gy', 'gz'), may hold values from 0 to 64, as said below
- gauss_opacity: float32 [8, 16, 64, 32], P('gx', 'gy', 'gz'), may hold values from 0.05 to 1
- gauss_count: int32 [8, 16, 64], P('gx', 'gy', 'gz'), may hold values from 8 to 32, as said below
Outputs:
- point_out: float32 [6144, 4, 128], P(('gx', 'gy', 'gz'))
- gauss_grad: float32 [8, 16, 64, 4, 32], P('gx', 'gy', 'gz')
The draws below stay inside these ranges and needn't reach their ends.
Inputs may be any that keep to these rules, and one draw needn't show every extreme that they name: `block_cell`: no two blocks name the same cell. Of the blocks that one device holds, at most 2 lie in the cells of any one brick (a brick is the 1 x 4 x 16 cells of one device of the grid). `block_count`: the valid points of a block are its first ones. `gauss_count`: the used slots of a cell are its first ones. `point_xyz`: every point lies in the cell of its block: each coordinate minus the cell's index lies in [0, 1]. `gauss_mean`: every centre, used or not, lies in its own cell: each coordinate minus the cell's index lies in [0, 1].
All inputs are finite; a program needn't handle non-finite values.
Results may differ from the reference program's by a relative error of at most 0.0003.
Values sent between devices are 32-bit elements; how exact they have to be, the bound alone decides.
A program may use at most 64 MiB of HBM per device.

```python
import math
import jax
import jax.numpy as jnp
from jax import lax

CX = 1
CY = 4
CZ = 16
NB = 48
GCAP = 32
PTS = 128
MOST = 2
CELLS_DEV = 64
BRICKS = 128
NX = 8
NY = 16
NZ = 64
BLOCKS = 6144


def route_cells(key):
    baseline_units = jax.random.fold_in(key, 7001)
    width_units = NB // MOST
    busy_run_count = max(1, BRICKS // 16)
    busy_units = min(BRICKS, CELLS_DEV // MOST)
    spare_units = BRICKS * width_units - busy_run_count * busy_units
    quiet_run_count = BRICKS - busy_run_count
    balanced_units = spare_units // quiet_run_count
    leftover_runs = spare_units % quiet_run_count
    run_owner = jax.random.permutation(jax.random.fold_in(baseline_units, 1), BRICKS).astype(jnp.int32)
    surplus_unit = (jax.random.permutation(jax.random.fold_in(baseline_units, 2), quiet_run_count) < leftover_runs).astype(jnp.int32)
    units_per_run = jnp.concatenate([jnp.full((busy_run_count,), busy_units, jnp.int32), balanced_units + surplus_unit])
    run_start = jnp.cumsum(units_per_run) - units_per_run
    scores = jax.random.randint(jax.random.fold_in(baseline_units, 3), (BRICKS, NB), 0, 1 << 12) * NB
    scores = scores + jnp.arange(NB, dtype=jnp.int32)[None, :]
    order_in = jnp.argsort(scores, axis=1).astype(jnp.int32)
    source = jnp.arange(BRICKS, dtype=jnp.int32)[:, None]
    unit_index = (order_in // MOST * BRICKS + source).reshape(-1)
    within = (order_in % MOST).reshape(-1)
    run_index = jnp.sum((run_start[None, :] <= unit_index[:, None]).astype(jnp.int32), axis=1) - 1
    arrival = (unit_index - run_start[run_index]) * MOST + within
    brick = run_owner[run_index]
    cell_scores = jax.random.randint(jax.random.fold_in(baseline_units, 4), (BRICKS, CELLS_DEV), 0, 1 << 12) * CELLS_DEV
    cell_scores = cell_scores + jnp.arange(CELLS_DEV, dtype=jnp.int32)[None, :]
    cell_order = jnp.argsort(cell_scores, axis=1).astype(jnp.int32)
    local_cell = cell_order[brick, arrival]
    bricks_y = NY // CY
    bricks_z = NZ // CZ
    brick_x = brick // (bricks_y * bricks_z)
    brick_y = brick // bricks_z % bricks_y
    brick_z = brick % bricks_z
    cell_x = brick_x * CX + local_cell // (CY * CZ)
    cell_y = brick_y * CY + local_cell // CZ % CY
    cell_z = brick_z * CZ + local_cell % CZ
    return ((cell_x * NY + cell_y) * NZ + cell_z).astype(jnp.int32)


def draw_block_cell(key, part):
    return route_cells(key)


def draw_block_count(key, part):
    counts = jax.random.randint(jax.random.fold_in(key, 21), (BLOCKS,), 1, PTS + 1)
    return counts.at[0].set(PTS).astype(jnp.int32)


def draw_gauss_count(key, part):
    counts = jax.random.randint(jax.random.fold_in(key, 31), (NX, NY, NZ), max(1, GCAP // 4), GCAP + 1)
    return counts.at[0, 0, 0].set(GCAP).astype(jnp.int32)


def draw_point_xyz(key, part):
    cells = route_cells(key)
    coords = jnp.stack([cells // (NY * NZ), cells // NZ % NY, cells % NZ], axis=1).astype(jnp.float32)
    noise = jax.random.uniform(jax.random.fold_in(key, 11), (BLOCKS, 3, PTS), jnp.float32)
    return coords[:, :, None] + noise


def draw_gauss_mean(key, part):
    grid = jnp.stack(jnp.meshgrid(jnp.arange(NX), jnp.arange(NY), jnp.arange(NZ), indexing='ij'), axis=-1)
    grid = grid.astype(jnp.float32)
    noise = jax.random.uniform(jax.random.fold_in(key, 41), (NX, NY, NZ, 3, GCAP), jnp.float32)
    return grid[..., :, None] + noise


def levels(stream_key, shape, pieces, least, top_value):
    level, own = 1.0, jax.random.fold_in(stream_key, 6)
    for axis_at, shards_of in pieces:
        draws = jnp.exp(jax.random.uniform(jax.random.fold_in(own, axis_at), (shards_of,), jnp.float32, least / len(pieces), top_value / len(pieces)))
        level = level * jnp.repeat(draws, shape[axis_at] // shards_of).reshape([-1 if axis == axis_at else 1 for axis in range(len(shape))])
    return level


def setup_inputs(seed: int = 0) -> dict:
    seeds = jax.random.split(jax.random.key(seed), 8)
    return {
        "point_xyz": draw_point_xyz(jax.random.fold_in(seeds[7], 71), 0),
        "point_weight": jnp.clip(jnp.exp(math.log(2.0) - 2.0794415 * jax.random.uniform(seeds[1], (BLOCKS, PTS), jnp.float32) ** levels(seeds[1], (BLOCKS, PTS), ((0, 128),), -0.2, 0.2)), 0.25, 2.0),
        "block_cell": draw_block_cell(jax.random.fold_in(seeds[7], 71), 0),
        "block_count": draw_block_count(jax.random.fold_in(seeds[7], 71), 0),
        "gauss_mean": draw_gauss_mean(jax.random.fold_in(seeds[7], 71), 0),
        "gauss_opacity": jnp.clip(jnp.exp(math.log(1.0) - 2.9957323 * jax.random.uniform(seeds[5], (NX, NY, NZ, GCAP), jnp.float32) ** levels(seeds[5], (NX, NY, NZ, GCAP), ((0, 8), (1, 4), (2, 4)), -0.2, 0.2)), 0.05, 1.0),
        "gauss_count": draw_gauss_count(jax.random.fold_in(seeds[7], 71), 0),
    }


kernel_width = 0.05
cutoff_sq = 0.5
floor_term = math.exp(-10.0)


def window(values, step_x, step_y, step_z, extent):
    anchor = jnp.zeros((), jnp.int32)
    corner = (step_x, step_y, step_z) + (anchor,) * (values.ndim - 3)
    return lax.dynamic_slice(values, corner, tuple(extent) + values.shape[3:])


def pair_block(own_items, own_inv, far_items, far_inv, second, with_far, with_density):
    delta_x = own_items[..., 0, :, None] - far_items[..., 0, None, :]
    delta_y = own_items[..., 1, :, None] - far_items[..., 1, None, :]
    delta_z = own_items[..., 2, :, None] - far_items[..., 2, None, :]
    distance = delta_x * delta_x + delta_y * delta_y + delta_z * delta_z
    falloff = jnp.exp(-distance / cutoff_sq)
    kernel = jnp.exp((falloff - 1.0) * (cutoff_sq / kernel_width))
    own_wt = own_items[..., 3, :, None]
    far_wt = far_items[..., 3, None, :]
    if not second:
        own_sum = jnp.sum(kernel * far_wt, axis=-1)
        far_sum = jnp.sum(kernel * own_wt, axis=-2) if with_far else None
        return own_sum, far_sum
    coupling = 2.0 * own_wt * far_wt * kernel * falloff * (own_inv[..., :, None] + far_inv[..., None, :])
    own_grad = jnp.stack([jnp.sum(coupling * delta_x, axis=-1), jnp.sum(coupling * delta_y, axis=-1),
                          jnp.sum(coupling * delta_z, axis=-1)], axis=-2)
    if with_density:
        own_density = jnp.sum(kernel * far_wt * far_inv[..., None, :], axis=-1)
        own_grad = jnp.concatenate([own_grad, own_density[..., None, :]], axis=-2)
    far_out = None
    if with_far:
        far_grad = -jnp.stack([jnp.sum(coupling * delta_x, axis=-2), jnp.sum(coupling * delta_y, axis=-2),
                               jnp.sum(coupling * delta_z, axis=-2)], axis=-2)
        far_density = jnp.sum(kernel * own_wt * own_inv[..., :, None], axis=-2)
        far_out = jnp.concatenate([far_grad, far_density[..., None, :]], axis=-2)
    return own_grad, far_out


def sweep_pairs(own_items, own_inv, far_grid, far_inv, second, with_density):
    extent = own_items.shape[:3]
    own_len = own_items.shape[-1]
    if second:
        own_acc = jnp.zeros(extent + ((4 if with_density else 3), own_len), jnp.float32)
    else:
        own_acc = jnp.zeros(extent + (own_len,), jnp.float32)

    def one_offset(offset, own_total):
        step_x = (offset // 9).astype(jnp.int32)
        step_y = ((offset // 3) % 3).astype(jnp.int32)
        step_z = (offset % 3).astype(jnp.int32)
        far_items = window(far_grid, step_x, step_y, step_z, extent)
        far_part_inv = window(far_inv, step_x, step_y, step_z, extent) if second else None
        own_part, unused = pair_block(own_items, own_inv, far_items, far_part_inv, second, False, with_density)
        return own_total + own_part

    return lax.fori_loop(0, 27, one_offset, own_acc)


def padded(values):
    return jnp.pad(values, ((1, 1), (1, 1), (1, 1)) + ((0, 0),) * (values.ndim - 3))


def planes(own_items, own_inv, far_grid, far_inv, second, with_density):
    def plane_terms(offset):
        own_plane = lax.dynamic_slice_in_dim(own_items, offset, 1, 0)
        far_plane = lax.dynamic_slice_in_dim(far_grid, offset, 3, 0)
        if second:
            inv_plane = lax.dynamic_slice_in_dim(own_inv, offset, 1, 0)
            far_inv_plane = lax.dynamic_slice_in_dim(far_inv, offset, 3, 0)
        else:
            inv_plane = None
            far_inv_plane = None
        result = sweep_pairs(own_plane, inv_plane, far_plane, far_inv_plane, second, with_density)
        return result[0]

    return lax.map(plane_terms, jnp.arange(NX, dtype=jnp.int32))


def reference(point_xyz, point_weight, block_cell, block_count, gauss_mean, gauss_opacity, gauss_count):
    is_valid = jnp.arange(PTS, dtype=jnp.int32)[None, :] < block_count[:, None]
    weights = jnp.where(is_valid, point_weight, 0.0)
    payload = jnp.concatenate([point_xyz, weights[:, None, :]], axis=1)
    points = jnp.zeros((NX * NY * NZ, 4, PTS), jnp.float32).at[block_cell].set(payload)
    points = points.reshape(NX, NY, NZ, 4, PTS)
    present = jnp.arange(GCAP, dtype=jnp.int32) < gauss_count[..., None]
    gaussians = jnp.concatenate([gauss_mean, jnp.where(present, gauss_opacity, 0.0)[..., None, :]], axis=3)
    total_p = floor_term + planes(points, None, padded(gaussians), None, False, False)
    total_g = floor_term + planes(gaussians, None, padded(points), None, False, False)
    inverse_p = 1.0 / total_p
    inverse_g = 1.0 / total_g
    gradient_p = planes(points, inverse_p, padded(gaussians), padded(inverse_g), True, False)
    gradient_g = planes(gaussians, inverse_g, padded(points), padded(inverse_p), True, True)
    loss_p = jnp.where(points[..., 3, :] > 0.0, -kernel_width * jnp.log(total_p), 0.0)
    cell_result = jnp.concatenate([loss_p[..., None, :], gradient_p], axis=3).reshape(NX * NY * NZ, 4, PTS)
    point_out = cell_result[block_cell]
    grad_opacity = jnp.where(present, -kernel_width * jnp.log(total_g) - kernel_width * gradient_g[..., 3, :], 0.0)
    gauss_grad = jnp.concatenate([gradient_g[..., :3, :], grad_opacity[..., None, :]], axis=3)
    return point_out, gauss_grad
```

```python
import functools
import math

import jax
import jax.numpy as jnp
from jax import lax
from jax.experimental import pallas as pl
from jax.experimental.pallas import tpu as pltpu
from jax.sharding import PartitionSpec as P

AXES = ("gx", "gy", "gz")
SX, SY, SZ = 8, 4, 4
BRICKS = SX * SY * SZ
CY, CZ = 4, 16
CELLS = CY * CZ
BLOCKS = 48
SLOTS = 32
LANES = 128
QUADS = CZ // 4
CHUNK = 32
GROUPS = CHUNK // 8
PER_CELL = LANES // CHUNK

LOG2E = 1.4426950408889634
WIDTH = 0.05
CUTOFF = 0.5
SHARP = CUTOFF / WIDTH * LOG2E
LIFT = math.log2(SHARP)
SCALE = math.sqrt(LOG2E / CUTOFF)
BACK = 2.0 / (SHARP * SCALE)
FLOOR = math.exp(-10.0)
GONE = -1.0e4
NUDGE = 4.0e-6

F32 = jnp.float32
I32 = jnp.int32
VMEM = pl.BlockSpec(memory_space=pltpu.VMEM)
SMEM = pl.BlockSpec(memory_space=pltpu.SMEM)
MESH = pl.DeviceIdType.MESH


def iota(shape, dim):
    return lax.broadcasted_iota(I32, shape, dim)


def here():
    return lax.axis_index("gx"), lax.axis_index("gy"), lax.axis_index("gz")


def place_of(brick):
    return (brick // (SY * SZ), brick // SZ % SY, brick % SZ)


def pack_kernel(cell_ref, count_ref, gcount_ref, xyz_ref, weight_ref, mean_ref, opacity_ref,
                out_ref, gauss_ref, slot_ref, used_ref):
    out_ref[...] = jnp.zeros_like(out_ref)

    def clear(i, carry):
        for u in range(8):
            used_ref[i * 8 + u] = 0
        return carry

    lax.fori_loop(0, BRICKS // 8, clear, 0)
    lane = iota((1, LANES), 1)
    row4 = iota((4, LANES), 0)
    lane4 = iota((4, LANES), 1)
    row8 = iota((8, LANES), 0)

    def one(b, carry):
        cell = cell_ref[b]
        cx = cell >> 10
        cy = (cell >> 6) & 15
        cz = cell & 63
        brick = (cx * SY + (cy >> 2)) * SZ + (cz >> 4)
        k = used_ref[brick]
        used_ref[brick] = k + 1
        slot_ref[b] = brick * 2 + k
        weight = jnp.where(lane < count_ref[b], weight_ref[pl.ds(b, 1), :], 0.0)
        rows = jnp.concatenate([xyz_ref[b], weight], axis=0)
        corner = jnp.where(row4 == 0, cx, jnp.where(row4 == 1, cy, cz))
        top = (corner + 1).astype(F32) - NUDGE
        rows = jnp.where((lane4 == 0) & (row4 < 3), jnp.minimum(rows, top), rows)
        both = jnp.concatenate([rows, rows], axis=0)
        out_ref[brick] = jnp.where((row8 >> 2) == k, both, out_ref[brick])
        return carry

    lax.fori_loop(0, BLOCKS, one, 0)
    for y in range(CY):
        for q in range(QUADS):
            mean = jnp.concatenate([mean_ref[y, 4 * q + r] for r in range(4)], axis=1)
            opacity = jnp.concatenate(
                [opacity_ref[y, 4 * q + r : 4 * q + r + 1, :] for r in range(4)], axis=1
            )
            base = y * CZ + 4 * q
            count = jnp.where(
                lane < 64,
                jnp.where(lane < 32, gcount_ref[base], gcount_ref[base + 1]),
                jnp.where(lane < 96, gcount_ref[base + 2], gcount_ref[base + 3]),
            )
            opacity = jnp.where((lane & 31) < count, opacity, 0.0)
            gauss_ref[y, q] = jnp.concatenate([mean, opacity, jnp.zeros((4, LANES), F32)], axis=0)


def pack(block_cell, block_count, gauss_count, xyz, weight, mean, opacity):
    return pl.pallas_call(
        pack_kernel,
        out_shape=(
            jax.ShapeDtypeStruct((BRICKS, 8, LANES), F32),
            jax.ShapeDtypeStruct((CY, QUADS, 8, LANES), F32),
            jax.ShapeDtypeStruct((BLOCKS,), I32),
        ),
        in_specs=[SMEM, SMEM, SMEM, VMEM, VMEM, VMEM, VMEM],
        out_specs=(VMEM, VMEM, SMEM),
        scratch_shapes=[pltpu.SMEM((BRICKS,), I32)],
        name="pack",
    )(block_cell, block_count, gauss_count, xyz, weight, mean, opacity)


OFFSETS = [
    (ox, oy, oz)
    for ox in (-1, 0, 1)
    for oy in (-1, 0, 1)
    for oz in (-1, 0, 1)
    if (ox, oy, oz) != (0, 0, 0)
]
OFFSETS.sort(key=lambda o: abs(o[1]) + abs(o[2]))


def neighbour(offset):
    gx, gy, gz = here()
    ox, oy, oz = offset
    return ((gx + ox + SX) % SX, (gy + oy + SY) % SY, (gz + oz + SZ) % SZ)


def greet_all():
    gx, gy, gz = here()
    me = (gx * SY + gy) * SZ + gz
    barrier = pltpu.get_barrier_semaphore()

    def signal(i, carry):
        pl.semaphore_signal(barrier, inc=1, device_id=place_of((me + i) % BRICKS), device_id_type=MESH)
        return carry

    lax.fori_loop(1, BRICKS, signal, 0)
    pl.semaphore_wait(barrier, BRICKS - 1)


def greet_near():
    barrier = pltpu.get_barrier_semaphore()
    for offset in OFFSETS:
        pl.semaphore_signal(barrier, inc=1, device_id=neighbour(offset), device_id_type=MESH)
    pl.semaphore_wait(barrier, len(OFFSETS))


def exchange_copy(src_ref, dst_ref, send_sem, recv_sem, i):
    gx, gy, gz = here()
    me = (gx * SY + gy) * SZ + gz
    peer = (me + i) % BRICKS
    return pltpu.make_async_remote_copy(
        src_ref=src_ref.at[peer],
        dst_ref=dst_ref.at[me],
        send_sem=send_sem.at[i],
        recv_sem=recv_sem.at[i],
        device_id=place_of(peer),
        device_id_type=MESH,
    )


def exchange_start(*refs):
    def step(i, carry):
        exchange_copy(*refs, i).start()
        return carry

    lax.fori_loop(1, BRICKS, step, 0)


def exchange_wait(*refs):
    def step(i, carry):
        exchange_copy(*refs, i).wait()
        return carry

    lax.fori_loop(1, BRICKS, step, 0)


def send_kernel(out_ref, gauss_ref, in_ref, halo_ref, asend, arecv, hsend, hrecv):
    gx, gy, gz = here()
    me = (gx * SY + gy) * SZ + gz
    greet_all()
    copies = []
    for d, (ox, oy, oz) in enumerate(OFFSETS):
        sy, ty, ny = (0, 1, CY) if oy == 0 else ((CY - 1, 0, 1) if oy > 0 else (0, CY + 1, 1))
        sq, tq, nq = (0, 1, QUADS) if oz == 0 else ((QUADS - 1, 0, 1) if oz > 0 else (0, QUADS + 1, 1))
        copies.append(
            pltpu.make_async_remote_copy(
                src_ref=gauss_ref.at[pl.ds(sy, ny), pl.ds(sq, nq)],
                dst_ref=halo_ref.at[1 - ox, pl.ds(ty, ny), pl.ds(tq, nq)],
                send_sem=hsend.at[d],
                recv_sem=hrecv.at[d],
                device_id=neighbour((ox, oy, oz)),
                device_id_type=MESH,
            )
        )
    exchange_start(out_ref, in_ref, asend, arecv)
    for copy in copies:
        copy.start()
    in_ref[me] = out_ref[me]
    for y in range(CY):
        for q in range(QUADS):
            halo_ref[1, y + 1, q + 1] = gauss_ref[y, q]
    for copy in copies:
        copy.wait()
    exchange_wait(out_ref, in_ref, asend, arecv)


def send(outgoing, gauss):
    return pl.pallas_call(
        send_kernel,
        out_shape=(
            jax.ShapeDtypeStruct((BRICKS, 8, LANES), F32),
            jax.ShapeDtypeStruct((3, CY + 2, QUADS + 2, 8, LANES), F32),
        ),
        in_specs=[VMEM, VMEM],
        out_specs=(VMEM, VMEM),
        scratch_shapes=[
            pltpu.SemaphoreType.DMA((BRICKS,)),
            pltpu.SemaphoreType.DMA((BRICKS,)),
            pltpu.SemaphoreType.DMA((26,)),
            pltpu.SemaphoreType.DMA((26,)),
        ],
        compiler_params=pltpu.CompilerParams(collective_id=0, has_side_effects=True),
        name="send",
    )(outgoing, gauss)


def spread(row):
    return jnp.broadcast_to(row, (8, LANES))


def first_kernel(in_ref, halo_ref, pts_ref, win_ref, part_ref, items_ref, slots_ref, total_ref,
                 meta_ref, metas_ref, turn_ref, zp_ref, acc_ref, sem):
    gx, gy, gz = here()
    row8 = iota((8, LANES), 0)
    lane8 = iota((8, LANES), 1)
    lane1 = iota((1, LANES), 1)

    def gather(i, found):
        for u in range(16):
            s = i * 16 + u
            tile = in_ref[s]
            mark = jnp.where((row8 & 3) == 3, (tile > 0.0).astype(F32), jnp.where(lane8 == 0, tile, 0.0))
            found = jnp.where(lane8 == s, jnp.sum(mark, axis=1, keepdims=True), found)
        return found

    found = lax.fori_loop(0, BRICKS // 16, gather, jnp.zeros((8, LANES), F32))
    cell = iota((CELLS, LANES), 0).astype(F32)
    lane64 = iota((CELLS, LANES), 1).astype(F32)
    slot = jnp.full((CELLS, LANES), -1.0, F32)
    count = jnp.zeros((CELLS, LANES), F32)
    for k in range(2):
        y0 = jnp.floor(found[4 * k + 1 : 4 * k + 2]) - (gy * CY).astype(F32)
        z0 = jnp.floor(found[4 * k + 2 : 4 * k + 3]) - (gz * CZ).astype(F32)
        size = found[4 * k + 3 : 4 * k + 4]
        label = jnp.where(size > 0.0, y0 * CZ + z0, -1.0)
        match = label == cell
        slot = jnp.where(match, 2.0 * lane64 + k, slot)
        count = jnp.where(match, jnp.broadcast_to(size, (CELLS, LANES)), count)
    slot = jnp.max(slot, axis=1, keepdims=True)
    count = jnp.max(count, axis=1, keepdims=True)
    meta_ref[...] = jnp.where(iota((CELLS, LANES), 1) == 0, slot, count).astype(I32)
    copy = pltpu.make_async_copy(meta_ref, metas_ref, sem)
    copy.start()

    acc_ref[...] = jnp.zeros_like(acc_ref)
    origin = jnp.where(row8 == 0, gx, jnp.where(row8 == 1, gy * CY + CY // 2, gz * CZ)).astype(F32)
    origin = jnp.where(row8 < 3, origin, 0.0)
    scale = jnp.where(row8 < 3, SCALE, 1.0).astype(F32)

    def windows(xy, carry):
        x = xy // (CY + 2)
        y = xy % (CY + 2)
        outside = ((x == 0) & (gx == 0)) | ((x == 2) & (gx == SX - 1))
        outside = outside | ((y == 0) & (gy == 0)) | ((y == CY + 1) & (gy == SY - 1))
        tiles = []
        for q in range(QUADS + 2):
            gone = outside
            if q == 0:
                gone = gone | (gz == 0)
            if q == QUADS + 1:
                gone = gone | (gz == SZ - 1)
            tile = halo_ref[x, y, q]
            opacity = jnp.where(gone, 0.0, tile)
            strength = jnp.where(opacity > 0.0, jnp.log2(jnp.maximum(opacity, 1e-30)) - SHARP, GONE)
            tiles.append(jnp.where(row8 == 3, strength, (tile - origin) * scale))
        for z in range(CZ):
            a, b = z // 4, z % 4
            if b == 0:
                tile = pltpu.roll(jnp.where(lane8 >= 96, tiles[a], tiles[a + 1]), 32, 1)
            elif b == 1:
                tile = tiles[a + 1]
            elif b == 2:
                tile = pltpu.roll(tiles[a + 1], 96, 1)
            else:
                tile = pltpu.roll(jnp.where(lane8 < 64, tiles[a + 2], tiles[a + 1]), 64, 1)
            tile = jnp.where((row8 == 3) & (lane8 >= 96), GONE, tile)
            tile = jnp.where(row8 == 2, tile - z * SCALE, tile)
            win_ref[z, xy] = tile
        return carry

    lax.fori_loop(0, 3 * (CY + 2), windows, 0)
    copy.wait()

    def listing(c, at):
        size = metas_ref[c, 1]
        slots_ref[c] = metas_ref[c, 0]
        for u in range(PER_CELL):
            items_ref[at + u] = c * PER_CELL + u
        return at + ((size + CHUNK - 1) >> (CHUNK.bit_length() - 1))

    total = lax.fori_loop(0, CELLS, listing, 0)
    total_ref[0] = total

    def prepare(i, carry):
        for u in range(4):
            c = i * 4 + u
            slot = slots_ref[c]
            safe = jnp.maximum(slot, 0)
            tile = in_ref[safe >> 1]
            tile = jnp.where((safe & 1) == 1, pltpu.roll(tile, 4, 0), tile)
            tile = jnp.where(slot >= 0, tile, 0.0)
            z = (c & (CZ - 1)).astype(F32)
            shift = origin + jnp.where(row8 == 2, z, 0.0)
            weight = jnp.where(tile > 0.0, jnp.log2(jnp.maximum(tile, 1e-30)), GONE)
            points = jnp.where(row8 == 3, weight, (tile - shift) * scale)
            points = jnp.where(row8 == 4, pltpu.roll(tile, 1, 0), points)
            pts_ref[c] = points
            turn_ref[c] = jnp.transpose(points)
        return carry

    lax.fori_loop(0, CELLS // 4, prepare, 0)

    def sweep(i, carry):
        item = items_ref[i]
        c = item >> (PER_CELL.bit_length() - 1)
        first = (item & (PER_CELL - 1)) * CHUNK
        y = c >> 4
        z = c & (CZ - 1)
        cols = [turn_ref[c, pl.ds(pl.multiple_of(first + 8 * g, 8), 8), :] for g in range(GROUPS)]
        feats = [[jnp.broadcast_to(col[:, f : f + 1], (8, LANES)) for f in range(4)] for col in cols]
        sums = [jnp.zeros((8, LANES), F32) for g in range(GROUPS)]
        for dx in range(3):
            for dy in range(3):
                xy = dx * (CY + 2) + y + dy
                mx, my, mz, la = [spread(win_ref[z, xy, f : f + 1, :]) for f in range(4)]
                far = None
                for g in range(GROUPS):
                    px, py, pz, lw = feats[g]
                    ex, ey, ez = px - mx, py - my, pz - mz
                    fall = jnp.exp2(LIFT - ex * ex - ey * ey - ez * ez)
                    term = jnp.exp2(fall + (la + lw))
                    sums[g] = sums[g] + term
                    far = term if far is None else far + term
                acc_ref[z, xy] = acc_ref[z, xy] + far
        for g in range(GROUPS):
            zp_ref[c, pl.ds(pl.multiple_of(first + 8 * g, 8), 8), :] = sums[g]
        return carry

    lax.fori_loop(0, total, sweep, 0)

    def fold(xy, carry):
        part_ref[xy] = fold_quads([acc_ref[z, xy] for z in range(CZ)], lane8)
        return carry

    lax.fori_loop(0, 3 * (CY + 2), fold, 0)

    def finish(i, carry):
        for u in range(4):
            c = i * 4 + u
            tile = pts_ref[c]
            weight = tile[4:5]
            valid = weight > 0.0
            density = jnp.sum(jnp.transpose(zp_ref[c]), axis=0, keepdims=True)
            total_p = FLOOR + jnp.where(valid, density / jnp.where(valid, weight, 1.0), 0.0)
            inverse = jnp.where(valid, 1.0 / total_p, 0.0)
            loss = jnp.where(valid, -WIDTH * jnp.log(total_p), 0.0)
            tile = jnp.where(row8 == 4, inverse, tile)
            pts_ref[c] = jnp.where(row8 == 5, loss, tile)
        return carry

    lax.fori_loop(0, CELLS // 4, finish, 0)


def fold_quads(tiles, lane8):
    quads = [jnp.zeros((8, LANES), F32) for q in range(QUADS + 2)]
    for z, tile in enumerate(tiles):
        a, b = z // 4, z % 4
        if b == 1:
            quads[a + 1] = quads[a + 1] + tile
        elif b == 2:
            quads[a + 1] = quads[a + 1] + pltpu.roll(tile, 32, 1)
        elif b == 0:
            moved = pltpu.roll(tile, 96, 1)
            quads[a] = quads[a] + jnp.where(lane8 >= 96, moved, 0.0)
            quads[a + 1] = quads[a + 1] + jnp.where(lane8 < 96, moved, 0.0)
        else:
            moved = pltpu.roll(tile, 64, 1)
            quads[a + 1] = quads[a + 1] + jnp.where(lane8 >= 64, moved, 0.0)
            quads[a + 2] = quads[a + 2] + jnp.where(lane8 < 64, moved, 0.0)
    rows = [jnp.sum(quad, axis=0, keepdims=True) for quad in quads]
    return jnp.concatenate(rows + [jnp.zeros((2, LANES), F32)], axis=0)


def first_sweep(incoming, halo):
    return pl.pallas_call(
        first_kernel,
        out_shape=(
            jax.ShapeDtypeStruct((CELLS, 8, LANES), F32),
            jax.ShapeDtypeStruct((CZ, 18, 8, LANES), F32),
            jax.ShapeDtypeStruct((18, 8, LANES), F32),
            jax.ShapeDtypeStruct((CELLS * PER_CELL + 8,), I32),
            jax.ShapeDtypeStruct((CELLS,), I32),
            jax.ShapeDtypeStruct((1,), I32),
        ),
        in_specs=[VMEM, VMEM],
        out_specs=(VMEM, VMEM, VMEM, SMEM, SMEM, SMEM),
        scratch_shapes=[
            pltpu.VMEM((CELLS, LANES), I32),
            pltpu.SMEM((CELLS, LANES), I32),
            pltpu.VMEM((CELLS, LANES, 8), F32),
            pltpu.VMEM((CELLS, LANES, LANES), F32),
            pltpu.VMEM((CZ, 18, 8, LANES), F32),
            pltpu.SemaphoreType.DMA,
        ],
        compiler_params=pltpu.CompilerParams(vmem_limit_bytes=48 * 1024 * 1024),
        name="first_sweep",
    )(incoming, halo)


def near_copies(part_of, box_ref, send_sem, recv_sem):
    copies = []
    for d, (ox, oy, oz) in enumerate(OFFSETS):
        y0, ny = (1, CY) if oy == 0 else ((CY + 1, 1) if oy > 0 else (0, 1))
        copies.append(
            pltpu.make_async_remote_copy(
                src_ref=part_of((1 + ox) * (CY + 2) + y0, ny),
                dst_ref=box_ref.at[d, pl.ds(0, ny)],
                send_sem=send_sem.at[d],
                recv_sem=recv_sem.at[d],
                device_id=neighbour((ox, oy, oz)),
                device_id_type=MESH,
            )
        )
    return copies


def quads_of(tile, oz):
    if oz == 0:
        return tile[1 : QUADS + 1]
    row = iota((QUADS, LANES), 0)
    if oz > 0:
        return jnp.where(row == 0, tile[QUADS + 1 : QUADS + 2], 0.0)
    return jnp.where(row == QUADS - 1, tile[0:1], 0.0)


def middle_kernel(part_ref, gauss_ref, inv_ref, loss_ref, box_ref, send1, recv1, send2, recv2):
    greet_near()
    copies = near_copies(lambda at, n: part_ref.at[pl.ds(at, n)], box_ref, send1, recv1)
    for copy in copies:
        copy.start()
    sums = [part_ref[(CY + 2) + y + 1][1 : QUADS + 1] for y in range(CY)]
    for d, (ox, oy, oz) in enumerate(OFFSETS):
        copies[d].wait_recv()
        for k in range(CY if oy == 0 else 1):
            y = k if oy == 0 else (0 if oy > 0 else CY - 1)
            sums[y] = sums[y] + quads_of(box_ref[d, k], oz)
    for y in range(CY):
        opacity = jnp.concatenate([gauss_ref[y, q][3:4] for q in range(QUADS)], axis=0)
        valid = opacity > 0.0
        total_g = FLOOR + jnp.where(valid, sums[y] / jnp.where(valid, opacity, 1.0), 0.0)
        blank = jnp.zeros((8 - QUADS, LANES), F32)
        inv_ref[1, (CY + 2) + y + 1] = jnp.concatenate([1.0 / total_g, blank], axis=0)
        loss = jnp.where(valid, -WIDTH * jnp.log(total_g), 0.0)
        loss_ref[y] = jnp.concatenate([loss, opacity], axis=0)
    back = []
    for d, (ox, oy, oz) in enumerate(OFFSETS):
        sy, ty, ny = (0, 1, CY) if oy == 0 else ((CY - 1, 0, 1) if oy > 0 else (0, CY + 1, 1))
        back.append(
            pltpu.make_async_remote_copy(
                src_ref=inv_ref.at[1, pl.ds((CY + 2) + 1 + sy, ny)],
                dst_ref=inv_ref.at[1 - oz, pl.ds((1 - ox) * (CY + 2) + ty, ny)],
                send_sem=send2.at[d],
                recv_sem=recv2.at[d],
                device_id=neighbour((ox, oy, oz)),
                device_id_type=MESH,
            )
        )
    for copy in back:
        copy.start()
    for copy in copies:
        copy.wait_send()
    for copy in back:
        copy.wait()


def middle(part, gauss):
    return pl.pallas_call(
        middle_kernel,
        out_shape=(
            jax.ShapeDtypeStruct((3, 18, 8, LANES), F32),
            jax.ShapeDtypeStruct((CY, 8, LANES), F32),
        ),
        in_specs=[VMEM, VMEM],
        out_specs=(VMEM, VMEM),
        scratch_shapes=[pltpu.VMEM((26, CY, 8, LANES), F32)] + [pltpu.SemaphoreType.DMA((26,))] * 4,
        compiler_params=pltpu.CompilerParams(collective_id=1, has_side_effects=True),
        name="middle",
    )(part, gauss)


def second_kernel(items_ref, slots_ref, total_ref, pts_ref, win_ref, inv_ref, reply_ref, part_ref,
                  turn_ref, ig_ref, grad_ref, acc_ref):
    row8 = iota((8, LANES), 0)
    lane8 = iota((8, LANES), 1)
    lane1 = iota((1, LANES), 1)
    reply_ref[...] = jnp.zeros_like(reply_ref)
    acc_ref[...] = jnp.zeros_like(acc_ref)

    def windows(xy, carry):
        own = inv_ref[1, xy]
        rows = [inv_ref[0, xy][QUADS - 1 : QUADS]] + [own[q : q + 1] for q in range(QUADS)]
        tile = jnp.concatenate(rows + [inv_ref[2, xy][0:1], jnp.zeros((2, LANES), F32)], axis=0)
        moved = [pltpu.roll(tile, 32, 1), tile, pltpu.roll(tile, 96, 1), pltpu.roll(tile, 64, 1)]
        for z in range(CZ):
            a, b = z // 4, z % 4
            row = moved[b][a + 1 : a + 2]
            if b == 0:
                row = jnp.where(lane1 < 32, moved[b][a : a + 1], row)
            elif b == 3:
                row = jnp.where(lane1 >= 64, moved[b][a + 2 : a + 3], row)
            ig_ref[z, xy] = spread(row)
        return carry

    lax.fori_loop(0, 18, windows, 0)

    def prepare(i, carry):
        for u in range(4):
            turn_ref[i * 4 + u] = jnp.transpose(pts_ref[i * 4 + u])
        return carry

    lax.fori_loop(0, CELLS // 4, prepare, 0)

    def sweep(i, carry):
        item = items_ref[i]
        c = item >> (PER_CELL.bit_length() - 1)
        first = (item & (PER_CELL - 1)) * CHUNK
        y = c >> 4
        z = c & (CZ - 1)
        cols = [turn_ref[c, pl.ds(pl.multiple_of(first + 8 * g, 8), 8), :] for g in range(GROUPS)]
        feats = [[jnp.broadcast_to(col[:, f : f + 1], (8, LANES)) for f in range(5)] for col in cols]
        sums = [[jnp.zeros((8, LANES), F32) for k in range(3)] for g in range(GROUPS)]
        for dx in range(3):
            for dy in range(3):
                xy = dx * (CY + 2) + y + dy
                mx, my, mz, la = [spread(win_ref[z, xy, f : f + 1, :]) for f in range(4)]
                ig = ig_ref[z, xy]
                far = [None] * 4
                for g in range(GROUPS):
                    px, py, pz, lw, ip = feats[g]
                    ex, ey, ez = px - mx, py - my, pz - mz
                    fall = jnp.exp2(LIFT - ex * ex - ey * ey - ez * ez)
                    term = jnp.exp2(fall + (la + lw))
                    pull = (term * fall) * (ip + ig)
                    parts = [pull * ex, pull * ey, pull * ez, term * ip]
                    for k in range(3):
                        sums[g][k] = sums[g][k] + parts[k]
                    far = [p if f is None else f + p for f, p in zip(far, parts)]
                for k in range(4):
                    acc_ref[z, xy, k] = acc_ref[z, xy, k] + far[k]
        for g in range(GROUPS):
            for k in range(3):
                grad_ref[k, c, pl.ds(pl.multiple_of(first + 8 * g, 8), 8), :] = sums[g][k]
        return carry

    lax.fori_loop(0, total_ref[0], sweep, 0)

    def fold(xy, carry):
        for k in range(4):
            part_ref[xy, k] = fold_quads([acc_ref[z, xy, k] for z in range(CZ)], lane8)
        return carry

    lax.fori_loop(0, 18, fold, 0)

    def finish(i, carry):
        for u in range(2):
            c = i * 2 + u
            tile = pts_ref[c]
            valid = tile[3:4] > 0.5 * GONE
            rows = [
                jnp.where(valid, jnp.sum(jnp.transpose(grad_ref[k, c]), axis=0, keepdims=True) * BACK, 0.0)
                for k in range(3)
            ]
            out = jnp.concatenate([tile[5:6]] + rows, axis=0)
            out = jnp.concatenate([out, out], axis=0)
            slot = slots_ref[c]
            safe = jnp.maximum(slot, 0)
            keep = ((row8 >> 2) == (safe & 1)) & (slot >= 0)
            reply_ref[safe >> 1] = jnp.where(keep, out, reply_ref[safe >> 1])
        return carry

    lax.fori_loop(0, CELLS // 2, finish, 0)


def second_sweep(items, slots, total, pts, win, inv):
    return pl.pallas_call(
        second_kernel,
        out_shape=(
            jax.ShapeDtypeStruct((BRICKS, 8, LANES), F32),
            jax.ShapeDtypeStruct((18, 4, 8, LANES), F32),
        ),
        in_specs=[SMEM, SMEM, SMEM, VMEM, VMEM, VMEM],
        out_specs=(VMEM, VMEM),
        scratch_shapes=[
            pltpu.VMEM((CELLS, LANES, 8), F32),
            pltpu.VMEM((CZ, 18, 8, LANES), F32),
            pltpu.VMEM((3, CELLS, LANES, LANES), F32),
            pltpu.VMEM((CZ, 18, 4, 8, LANES), F32),
        ],
        compiler_params=pltpu.CompilerParams(vmem_limit_bytes=56 * 1024 * 1024),
        name="second_sweep",
    )(items, slots, total, pts, win, inv)


def last_kernel(reply_ref, part_ref, loss_ref, ans_ref, grad_ref, box_ref, asend, arecv, hsend, hrecv):
    gx, gy, gz = here()
    me = (gx * SY + gy) * SZ + gz
    greet_all()
    copies = near_copies(lambda at, n: part_ref.at[pl.ds(at, n)], box_ref, hsend, hrecv)
    for copy in copies:
        copy.start()
    exchange_start(reply_ref, ans_ref, asend, arecv)
    ans_ref[me] = reply_ref[me]
    sums = [[part_ref[(CY + 2) + y + 1, k][1 : QUADS + 1] for k in range(4)] for y in range(CY)]
    for d, (ox, oy, oz) in enumerate(OFFSETS):
        copies[d].wait_recv()
        for j in range(CY if oy == 0 else 1):
            y = j if oy == 0 else (0 if oy > 0 else CY - 1)
            for k in range(4):
                sums[y][k] = sums[y][k] + quads_of(box_ref[d, j, k], oz)
    for y in range(CY):
        loss = loss_ref[y][0:QUADS]
        opacity = loss_ref[y][QUADS : 2 * QUADS]
        valid = opacity > 0.0
        for k in range(3):
            grad_ref[y, k] = jnp.where(valid, sums[y][k] * (-BACK), 0.0)
        dense = sums[y][3] / jnp.where(valid, opacity, 1.0)
        grad_ref[y, 3] = jnp.where(valid, loss - WIDTH * dense, 0.0)
    for copy in copies:
        copy.wait_send()
    exchange_wait(reply_ref, ans_ref, asend, arecv)


def last(reply, part, loss):
    return pl.pallas_call(
        last_kernel,
        out_shape=(
            jax.ShapeDtypeStruct((BRICKS, 8, LANES), F32),
            jax.ShapeDtypeStruct((CY, 4, QUADS, LANES), F32),
        ),
        in_specs=[VMEM, VMEM, VMEM],
        out_specs=(VMEM, VMEM),
        scratch_shapes=[
            pltpu.VMEM((26, CY, 4, 8, LANES), F32),
            pltpu.SemaphoreType.DMA((BRICKS,)),
            pltpu.SemaphoreType.DMA((BRICKS,)),
            pltpu.SemaphoreType.DMA((26,)),
            pltpu.SemaphoreType.DMA((26,)),
        ],
        compiler_params=pltpu.CompilerParams(collective_id=2, has_side_effects=True),
        name="last",
    )(reply, part, loss)


def place_kernel(slot_ref, ans_ref, grad_ref, point_ref, gauss_ref):
    def one(b, carry):
        slot = slot_ref[b]
        tile = ans_ref[slot >> 1]
        tile = jnp.where((slot & 1) == 1, pltpu.roll(tile, 4, 0), tile)
        point_ref[b] = tile[0:4]
        return carry

    lax.fori_loop(0, BLOCKS, one, 0)
    for y in range(CY):
        rows = [grad_ref[y, k] for k in range(4)]
        for q in range(QUADS):
            tile = jnp.concatenate([row[q : q + 1] for row in rows], axis=0)
            for r in range(4):
                gauss_ref[0, y, 4 * q + r] = tile[:, SLOTS * r : SLOTS * r + SLOTS]


def place(slots, answer, grad):
    return pl.pallas_call(
        place_kernel,
        out_shape=(
            jax.ShapeDtypeStruct((BLOCKS, 4, LANES), F32),
            jax.ShapeDtypeStruct((1, CY, CZ, 4, SLOTS), F32),
        ),
        in_specs=[SMEM, VMEM, VMEM],
        out_specs=(VMEM, VMEM),
        name="place",
    )(slots, answer, grad)


def on_device(point_xyz, point_weight, block_cell, block_count, gauss_mean, gauss_opacity, gauss_count):
    outgoing, gauss, slots = pack(
        block_cell,
        block_count,
        gauss_count.reshape(CELLS),
        point_xyz,
        point_weight,
        gauss_mean.reshape(CY, CZ, 3, SLOTS),
        gauss_opacity.reshape(CY, CZ, SLOTS),
    )
    incoming, halo = send(outgoing, gauss)
    pts, win, part, items, cell_slots, total = first_sweep(incoming, halo)
    inv, loss = middle(part, gauss)
    reply, part = second_sweep(items, cell_slots, total, pts, win, inv)
    answer, grad = last(reply, part, loss)
    return place(slots, answer, grad)


def solution(mesh):
    return jax.shard_map(
        on_device,
        mesh=mesh,
        in_specs=(
            P(AXES, None, None),
            P(AXES, None),
            P(AXES),
            P(AXES),
            P("gx", "gy", "gz", None, None),
            P("gx", "gy", "gz", None),
            P("gx", "gy", "gz"),
        ),
        out_specs=(P(AXES, None, None), P("gx", "gy", "gz", None, None)),
        check_vma=False,
    )
```

```python
import functools
import math

import jax
import jax.numpy as jnp
from jax import lax
from jax.experimental import pallas as pl
from jax.experimental.pallas import tpu as pltpu
from jax.sharding import PartitionSpec as P

AXES = ("gx", "gy", "gz")
SX, SY, SZ = 8, 4, 4
BRICKS = SX * SY * SZ
CY, CZ = 4, 16
CELLS = CY * CZ
BLOCKS = 48
SLOTS = 32
LANES = 128
QUADS = CZ // 4
GROUPS = 4
CHUNKS = LANES // (8 * GROUPS)
ITEMS = CELLS * CHUNKS
TILES = 7
ROWS = CY + 2
COLUMNS = 3 * ROWS

LOG2E = 1.4426950408889634
WIDTH = 0.05
CUTOFF = 0.5
SHARP = CUTOFF / WIDTH * LOG2E
LIFT = math.log2(SHARP)
SCALE = math.sqrt(LOG2E / CUTOFF)
BACK = 2.0 / (SHARP * SCALE)
FLOOR = math.exp(-10.0)
GONE = -1.0e4
NUDGE = 4.0e-6

F32 = jnp.float32
I32 = jnp.int32
VMEM = pl.BlockSpec(memory_space=pltpu.VMEM)
SMEM = pl.BlockSpec(memory_space=pltpu.SMEM)
MESH = pl.DeviceIdType.MESH


def iota(shape, dim):
    return lax.broadcasted_iota(I32, shape, dim)


def here():
    return lax.axis_index("gx"), lax.axis_index("gy"), lax.axis_index("gz")


def place_of(brick):
    return (brick // (SY * SZ), brick // SZ % SY, brick % SZ)


OFFSETS = [
    (ox, oy, oz)
    for ox in (-1, 0, 1)
    for oy in (-1, 0, 1)
    for oz in (-1, 0, 1)
    if (ox, oy, oz) != (0, 0, 0)
]
OFFSETS.sort(key=lambda o: abs(o[1]) + abs(o[2]))


def neighbour(offset):
    gx, gy, gz = here()
    ox, oy, oz = offset
    return ((gx + ox + SX) % SX, (gy + oy + SY) % SY, (gz + oz + SZ) % SZ)


def exchange_copy(src_ref, dst_ref, send_sem, recv_sem, i):
    gx, gy, gz = here()
    me = (gx * SY + gy) * SZ + gz
    peer = (me + i) % BRICKS
    return pltpu.make_async_remote_copy(
        src_ref=src_ref.at[peer],
        dst_ref=dst_ref.at[me],
        send_sem=send_sem.at[i],
        recv_sem=recv_sem.at[i],
        device_id=place_of(peer),
        device_id_type=MESH,
    )


def exchange_start(*refs):
    def step(i, carry):
        exchange_copy(*refs, i).start()
        return carry

    lax.fori_loop(1, BRICKS, step, 0)


def exchange_wait(*refs):
    def step(i, carry):
        exchange_copy(*refs, i).wait()
        return carry

    lax.fori_loop(1, BRICKS, step, 0)


def spread(row):
    return jnp.broadcast_to(row, (8, LANES))


def signal_all():
    gx, gy, gz = here()
    me = (gx * SY + gy) * SZ + gz
    barrier = pltpu.get_barrier_semaphore()

    def signal(i, carry):
        pl.semaphore_signal(barrier, inc=1, device_id=place_of((me + i) % BRICKS), device_id_type=MESH)
        return carry

    lax.fori_loop(1, BRICKS, signal, 0)


def pack_points(cell_ref, count_ref, xyz_ref, weight_ref, pay_ref, out_ref, home_ref, homes_ref, sem):
    lane = iota((1, LANES), 1)
    row4 = iota((4, LANES), 0)
    lane4 = iota((4, LANES), 1)
    row8 = iota((8, LANES), 0)

    def payload(b, carry):
        first, second = carry
        cell = cell_ref[b]
        cx = cell >> 10 & 7
        cy = (cell >> 6) & 15
        cz = cell & 63
        brick = (cx * SY + (cy >> 2)) * SZ + (cz >> 4)
        hit = lane == brick
        later = hit & (first < BLOCKS)
        second = jnp.where(later, b, second)
        first = jnp.where(hit & (first == BLOCKS), b, first)
        weight = jnp.where(lane < count_ref[b], weight_ref[pl.ds(b, 1), :], 0.0)
        rows = jnp.concatenate([xyz_ref[b], weight], axis=0)
        corner = jnp.where(row4 == 0, cx, jnp.where(row4 == 1, cy, cz))
        top = (corner + 1).astype(F32) - NUDGE
        rows = jnp.where((lane4 == 0) & (row4 < 3), jnp.minimum(rows, top), rows)
        pay_ref[b] = jnp.concatenate([rows, rows], axis=0)
        return first, second

    none = jnp.full((1, LANES), BLOCKS, I32)
    first, second = lax.fori_loop(0, BLOCKS, payload, (none, none))
    pay_ref[BLOCKS] = jnp.zeros((8, LANES), F32)
    home_ref[...] = jnp.where(row8 == 0, first, second)
    copy = pltpu.make_async_copy(home_ref, homes_ref, sem)
    copy.start()
    copy.wait()

    def put(i, carry):
        for u in range(4):
            d = i * 4 + u
            first = jnp.clip(homes_ref[0, d], 0, BLOCKS)
            second = jnp.clip(homes_ref[1, d], 0, BLOCKS)
            out_ref[d] = jnp.where(row8 < 4, pay_ref[first], pay_ref[second])
        return carry

    lax.fori_loop(0, BRICKS // 4, put, 0)


def pack_gauss(gcount_ref, mean_ref, opacity_ref, gauss_ref):
    lane = iota((1, LANES), 1)
    for y in range(CY):
        for q in range(QUADS):
            mean = jnp.concatenate([mean_ref[0, y, 4 * q + r] for r in range(4)], axis=1)
            opacity = jnp.concatenate(
                [opacity_ref[0, y, 4 * q + r : 4 * q + r + 1, :] for r in range(4)], axis=1
            )
            have = [gcount_ref[0, y, 4 * q + r] for r in range(4)]
            count = jnp.where(
                lane < 64,
                jnp.where(lane < 32, have[0], have[1]),
                jnp.where(lane < 96, have[2], have[3]),
            )
            opacity = jnp.where((lane & 31) < count, opacity, 0.0)
            gauss_ref[y, q] = jnp.concatenate([mean, opacity, jnp.zeros((4, LANES), F32)], axis=0)


def side(o, last):
    if o == 0:
        return 0, 1, last + 1
    return (last, 0, 1) if o > 0 else (0, last + 2, 1)


def halo_copies(gauss_ref, halo_ref, send_sem, recv_sem):
    copies = []
    for d, (ox, oy, oz) in enumerate(OFFSETS):
        sy, ty, ny = side(oy, CY - 1)
        sq, tq, nq = side(oz, QUADS - 1)
        copies.append(
            pltpu.make_async_remote_copy(
                src_ref=gauss_ref.at[pl.ds(sy, ny), pl.ds(sq, nq)],
                dst_ref=halo_ref.at[1 - ox, pl.ds(ty, ny), pl.ds(tq, nq)],
                send_sem=send_sem.at[d],
                recv_sem=recv_sem.at[d],
                device_id=neighbour((ox, oy, oz)),
                device_id_type=MESH,
            )
        )
    return copies


def near_copies(part_ref, box_ref, send_sem, recv_sem):
    copies = []
    for d, (ox, oy, oz) in enumerate(OFFSETS):
        y0, ny = (1, CY) if oy == 0 else ((CY + 1, 1) if oy > 0 else (0, 1))
        copies.append(
            pltpu.make_async_remote_copy(
                src_ref=part_ref.at[pl.ds((1 + ox) * ROWS + y0, ny)],
                dst_ref=box_ref.at[d, pl.ds(0, ny)],
                send_sem=send_sem.at[d],
                recv_sem=recv_sem.at[d],
                device_id=neighbour((ox, oy, oz)),
                device_id_type=MESH,
            )
        )
    return copies


def inverse_copies(inv_ref, send_sem, recv_sem):
    copies = []
    for d, (ox, oy, oz) in enumerate(OFFSETS):
        sy, ty, ny = side(oy, CY - 1)
        copies.append(
            pltpu.make_async_remote_copy(
                src_ref=inv_ref.at[1, pl.ds(ROWS + 1 + sy, ny)],
                dst_ref=inv_ref.at[1 - oz, pl.ds((1 - ox) * ROWS + ty, ny)],
                send_sem=send_sem.at[d],
                recv_sem=recv_sem.at[d],
                device_id=neighbour((ox, oy, oz)),
                device_id_type=MESH,
            )
        )
    return copies


def feature_windows(halo_ref, win_ref, origin, scale):
    gx, gy, gz = here()
    row8 = iota((8, LANES), 0)
    lane8 = iota((8, LANES), 1)

    def windows(xy, carry):
        x = xy // ROWS
        y = xy % ROWS
        outside = ((x == 0) & (gx == 0)) | ((x == 2) & (gx == SX - 1))
        outside = outside | ((y == 0) & (gy == 0)) | ((y == CY + 1) & (gy == SY - 1))
        tiles = []
        for q in range(QUADS + 2):
            gone = outside
            if q == 0:
                gone = gone | (gz == 0)
            if q == QUADS + 1:
                gone = gone | (gz == SZ - 1)
            tile = halo_ref[x, y, q]
            opacity = jnp.where(gone, 0.0, tile)
            strength = jnp.where(opacity > 0.0, jnp.log2(jnp.maximum(opacity, 1e-30)) - SHARP, GONE)
            tiles.append(jnp.where(row8 == 3, strength, (tile - origin) * scale))
        for z in range(CZ):
            a, b = z // 4, z % 4
            if b == 0:
                tile = pltpu.roll(jnp.where(lane8 >= 96, tiles[a], tiles[a + 1]), 32, 1)
            elif b == 1:
                tile = tiles[a + 1]
            elif b == 2:
                tile = pltpu.roll(tiles[a + 1], 96, 1)
            else:
                tile = pltpu.roll(jnp.where(lane8 < 64, tiles[a + 2], tiles[a + 1]), 64, 1)
            tile = jnp.where((row8 == 3) & (lane8 >= 96), GONE, tile)
            win_ref[z, xy] = jnp.where(row8 == 2, tile - z * SCALE, tile)
        return carry

    lax.fori_loop(0, COLUMNS, windows, 0)


def inverse_windows(inv_ref, win_ref):
    row8 = iota((8, LANES), 0)
    lane1 = iota((1, LANES), 1)

    def windows(xy, carry):
        own = inv_ref[1, xy]
        rows = [inv_ref[0, xy][QUADS - 1 : QUADS]] + [own[q : q + 1] for q in range(QUADS)]
        tile = jnp.concatenate(rows + [inv_ref[2, xy][0:1], jnp.zeros((2, LANES), F32)], axis=0)
        moved = [pltpu.roll(tile, 32, 1), tile, pltpu.roll(tile, 96, 1), pltpu.roll(tile, 64, 1)]
        for z in range(CZ):
            a, b = z // 4, z % 4
            row = moved[b][a + 1 : a + 2]
            if b == 0:
                row = jnp.where(lane1 < 32, moved[b][a : a + 1], row)
            elif b == 3:
                row = jnp.where(lane1 >= 64, moved[b][a + 2 : a + 3], row)
            win_ref[z, xy] = jnp.where(row8 == 4, row, win_ref[z, xy])
        return carry

    lax.fori_loop(0, COLUMNS, windows, 0)


TRIPLES = [(x, dy, divmod(3 * (3 * x + dy), 4)) for x in range(3) for dy in range(3)]


def compose(win_ref, tile_ref):
    lane8 = iota((8, LANES), 1)

    def one(c, carry):
        y = c // CZ
        z = c % CZ
        tiles = [None] * (TILES + 1)
        for x, dy, (j, p) in TRIPLES:
            piece = win_ref[z, x * ROWS + y + dy]
            if p:
                piece = pltpu.roll(piece, 32 * p, 1)
                tiles[j] = jnp.where(lane8 < 32 * p, tiles[j], piece)
            else:
                tiles[j] = piece
            tiles[j + 1] = piece
        for j in range(TILES):
            tile_ref[c, j] = tiles[j]
        return carry

    lax.fori_loop(0, CELLS, one, 0)


def uncompose(acc_ref, wide_ref, count):
    row8 = iota((8, LANES), 0)
    lane8 = iota((8, LANES), 1)
    wide_ref[...] = jnp.zeros_like(wide_ref)

    def one(c, carry):
        y = c // CZ
        z = c % CZ
        tiles = []
        for j in range(TILES):
            rows = [jnp.sum(acc_ref[c, j * count + k], axis=0, keepdims=True) for k in range(count)]
            tile = spread(rows[0])
            for k in range(1, count):
                tile = jnp.where((row8 & 3) == k, rows[k], tile)
            tiles.append(tile)
        for x, dy, (j, p) in TRIPLES:
            tile = tiles[j]
            if p:
                tile = pltpu.roll(jnp.where(lane8 >= 32 * p, tiles[j], tiles[j + 1]), LANES - 32 * p, 1)
            at = x * ROWS + y + dy
            wide_ref[z, at] = wide_ref[z, at] + jnp.where(lane8 < 96, tile, 0.0)
        return carry

    lax.fori_loop(0, CELLS, one, 0)


def fold_quads(wide_ref, xy, lane8):
    quads = [jnp.zeros((8, LANES), F32) for q in range(QUADS + 2)]
    for z in range(CZ):
        tile = wide_ref[z, xy]
        a, b = z // 4, z % 4
        if b == 1:
            quads[a + 1] = quads[a + 1] + tile
        elif b == 2:
            quads[a + 1] = quads[a + 1] + pltpu.roll(tile, 32, 1)
        elif b == 0:
            moved = pltpu.roll(tile, 96, 1)
            quads[a] = quads[a] + jnp.where(lane8 >= 96, moved, 0.0)
            quads[a + 1] = quads[a + 1] + jnp.where(lane8 < 96, moved, 0.0)
        else:
            moved = pltpu.roll(tile, 64, 1)
            quads[a + 1] = quads[a + 1] + jnp.where(lane8 >= 64, moved, 0.0)
            quads[a + 2] = quads[a + 2] + jnp.where(lane8 < 64, moved, 0.0)
    return quads


def decode(in_ref, meta_ref, metas_ref, sem):
    gx, gy, gz = here()
    row8 = iota((8, LANES), 0)
    lane8 = iota((8, LANES), 1)

    def gather(i, found):
        for u in range(32):
            s = i * 32 + u
            found = jnp.where(lane8 == s, jnp.broadcast_to(in_ref[s][:, 0:1], (8, LANES)), found)
        return found

    found = lax.fori_loop(0, BRICKS // 32, gather, jnp.zeros((8, LANES), F32))
    cell = iota((CELLS, LANES), 0).astype(F32)
    lane64 = iota((CELLS, LANES), 1).astype(F32)
    slot = jnp.full((CELLS, LANES), -1.0, F32)
    labels = []
    for k in range(2):
        y0 = jnp.floor(found[4 * k + 1 : 4 * k + 2]) - (gy * CY).astype(F32)
        z0 = jnp.floor(found[4 * k + 2 : 4 * k + 3]) - (gz * CZ).astype(F32)
        label = jnp.where(found[4 * k + 3 : 4 * k + 4] > 0.0, y0 * CZ + z0, -1.0)
        slot = jnp.where(label == cell, 2.0 * lane64 + k, slot)
        labels.append(jnp.clip(label, 0.0, CELLS - 1.0))
    slot = jnp.max(slot, axis=1, keepdims=True)
    meta_ref[pl.ds(0, CELLS), :] = jnp.broadcast_to(slot, (CELLS, LANES)).astype(I32)
    meta_ref[pl.ds(CELLS, 8), :] = jnp.where(row8 == 0, labels[0], labels[1]).astype(I32)
    copy = pltpu.make_async_copy(meta_ref, metas_ref, sem)
    copy.start()
    copy.wait()


def take_points(in_ref, metas_ref, turn_ref, origin, scale):
    row8 = iota((8, LANES), 0)

    def prepare(i, carry):
        for u in range(4):
            c = i * 4 + u
            slot = metas_ref[c, 0]
            safe = jnp.clip(slot, 0, 2 * BRICKS - 1)
            tile = in_ref[safe >> 1]
            tile = jnp.where((safe & 1) == 1, pltpu.roll(tile, 4, 0), tile)
            tile = jnp.where(slot >= 0, tile, 0.0)
            shift = origin + jnp.where(row8 == 2, (c % CZ).astype(F32), 0.0)
            weight = jnp.where(tile > 0.0, jnp.log2(jnp.maximum(tile, 1e-30)), GONE)
            turn_ref[c] = jnp.transpose(jnp.where(row8 == 3, weight, (tile - shift) * scale))
        return carry

    lax.fori_loop(0, CELLS // 4, prepare, 0)


def rows_of(i):
    return i // CHUNKS, i % CHUNKS * (8 * GROUPS)


def broadcasts(turn_ref, i):
    c, first = rows_of(i)
    cols = [turn_ref[c, pl.ds(pl.multiple_of(first + 8 * g, 8), 8), :] for g in range(GROUPS)]
    return [[jnp.broadcast_to(col[:, f : f + 1], (8, LANES)) for f in range(4)] for col in cols]


def keep_features(ahead_ref, feats):
    for g in range(GROUPS):
        for f in range(4):
            ahead_ref[4 * g + f] = feats[g][f]


def first_pass(turn_ref, tile_ref, ahead_ref, late_ref, zp_ref, acc_ref):
    acc_ref[:, 0:TILES] = jnp.zeros((CELLS, TILES, 8, LANES), F32)
    keep_features(ahead_ref, broadcasts(turn_ref, 0))
    for g in range(GROUPS):
        late_ref[g] = jnp.zeros((8, LANES), F32)

    def settle(i):
        for g in range(GROUPS):
            total = jnp.sum(late_ref[g], axis=1, keepdims=True)
            zp_ref[i * GROUPS + g] = jnp.broadcast_to(total, (8, LANES))

    def sweep(i, carry):
        feats = [[ahead_ref[4 * g + f] for f in range(4)] for g in range(GROUPS)]
        settle((i + ITEMS - 1) % ITEMS)
        following = broadcasts(turn_ref, jnp.minimum(i + 1, ITEMS - 1))
        c, first = rows_of(i)
        sums = [None] * GROUPS
        for j in range(TILES):
            mx, my, mz, la = [spread(tile_ref[c, j, f : f + 1, :]) for f in range(4)]
            far = None
            for g in range(GROUPS):
                px, py, pz, lw = feats[g]
                ex, ey, ez = px - mx, py - my, pz - mz
                fall = jnp.exp2(LIFT - ex * ex - ey * ey - ez * ez)
                term = jnp.exp2(fall + (la + lw))
                sums[g] = term if sums[g] is None else sums[g] + term
                far = term if far is None else far + term
            acc_ref[c, j] = acc_ref[c, j] + far
        for g in range(GROUPS):
            late_ref[g] = sums[g]
        keep_features(ahead_ref, following)
        return carry

    lax.fori_loop(0, ITEMS, sweep, 0)
    settle(ITEMS - 1)


def second_pass(turn_ref, tile_ref, ahead_ref, late_ref, zp_ref, acc_ref, stage_ref):
    acc_ref[...] = jnp.zeros_like(acc_ref)
    keep_features(ahead_ref, broadcasts(turn_ref, 0))
    for g in range(4 * GROUPS):
        late_ref[g] = jnp.ones((8, LANES), F32)
    lane = iota((8, LANES), 1) & 3

    def settle(i):
        c, first = rows_of(i)
        for g in range(GROUPS):
            out = (WIDTH * jnp.log(late_ref[4 * g + 3]))
            for k in range(3):
                total = jnp.sum(late_ref[4 * g + k], axis=1, keepdims=True) * BACK
                out = jnp.where(lane == k + 1, total, out)
            stage_ref[c, pl.ds(pl.multiple_of(first + 8 * g, 8), 8), :] = out[:, 0:8]

    def sweep(i, carry):
        feats = [[ahead_ref[4 * g + f] for f in range(4)] for g in range(GROUPS)]
        settle((i + ITEMS - 1) % ITEMS)
        following = broadcasts(turn_ref, jnp.minimum(i + 1, ITEMS - 1))
        c, first = rows_of(i)
        inverse = []
        for g in range(GROUPS):
            lw = feats[g][3]
            total = FLOOR + zp_ref[i * GROUPS + g] * jnp.exp2(-jnp.maximum(lw, -64.0))
            inverse.append(jnp.where(lw > 0.5 * GONE, 1.0 / total, 1.0))
        sums = [[None] * 3 for g in range(GROUPS)]
        for j in range(TILES):
            mx, my, mz, la, ig = [spread(tile_ref[c, j, f : f + 1, :]) for f in range(5)]
            far = [None] * 4
            for g in range(GROUPS):
                px, py, pz, lw = feats[g]
                ex, ey, ez = px - mx, py - my, pz - mz
                fall = jnp.exp2(LIFT - ex * ex - ey * ey - ez * ez)
                term = jnp.exp2(fall + (la + lw))
                pull = (term * fall) * (inverse[g] + ig)
                parts = [pull * ex, pull * ey, pull * ez, term * inverse[g]]
                sums[g] = [p if s is None else s + p for s, p in zip(sums[g], parts)]
                far = [p if s is None else s + p for s, p in zip(far, parts)]
            for k in range(4):
                acc_ref[c, 4 * j + k] = acc_ref[c, 4 * j + k] + far[k]
        for g in range(GROUPS):
            for k in range(3):
                late_ref[4 * g + k] = sums[g][k]
            late_ref[4 * g + 3] = inverse[g]
        keep_features(ahead_ref, following)
        return carry

    lax.fori_loop(0, ITEMS, sweep, 0)
    settle(ITEMS - 1)


def answer_points(stage_ref, res_ref, metas_ref, reply_ref):
    row8 = iota((8, LANES), 0)

    def turn(i, carry):
        for u in range(4):
            res_ref[i * 4 + u] = jnp.transpose(stage_ref[i * 4 + u])
        return carry

    lax.fori_loop(0, CELLS // 4, turn, 0)

    def put(i, carry):
        for u in range(4):
            s = i * 4 + u
            first = jnp.clip(metas_ref[CELLS, s], 0, CELLS - 1)
            second = jnp.clip(metas_ref[CELLS + 1, s], 0, CELLS - 1)
            reply_ref[s] = jnp.where(row8 < 4, res_ref[first], res_ref[second])
        return carry

    lax.fori_loop(0, BRICKS // 4, put, 0)


def quads_of(tile, oz):
    if oz == 0:
        return tile[1 : QUADS + 1]
    row = iota((QUADS, LANES), 0)
    if oz > 0:
        return jnp.where(row == 0, tile[QUADS + 1 : QUADS + 2], 0.0)
    return jnp.where(row == QUADS - 1, tile[0:1], 0.0)


def owner_row(oy, k):
    return k if oy == 0 else (0 if oy > 0 else CY - 1)


def kernel(cell_ref, count_ref, gcount_ref, xyz_ref, weight_ref, mean_ref, opacity_ref,
           point_ref, grad_ref,
           pay_ref, out_ref, in_ref, home_ref, homes_ref, gauss_ref, halo_ref, win_ref, tile_ref,
           meta_ref, metas_ref, turn_ref, ahead_ref, late_ref, zp_ref, acc_ref, wide_ref, part_ref,
           box_ref, inv_ref, loss_ref, stage_ref, res_ref, reply_ref, ans_ref, pull_ref, pulls_ref,
           local_sem, asend, arecv, bsend, brecv, near_sem):
    gx, gy, gz = here()
    me = (gx * SY + gy) * SZ + gz
    row8 = iota((8, LANES), 0)
    lane8 = iota((8, LANES), 1)
    signal_all()
    pack_gauss(gcount_ref, mean_ref, opacity_ref, gauss_ref)
    pack_points(cell_ref, count_ref, xyz_ref, weight_ref, pay_ref, out_ref, home_ref, homes_ref, local_sem.at[0])
    pl.semaphore_wait(pltpu.get_barrier_semaphore(), BRICKS - 1)
    halo = halo_copies(gauss_ref, halo_ref, near_sem.at[0], near_sem.at[1])
    for copy in halo:
        copy.start()
    exchange_start(out_ref, in_ref, asend, arecv)
    in_ref[me] = out_ref[me]
    for y in range(CY):
        for q in range(QUADS):
            halo_ref[1, y + 1, q + 1] = gauss_ref[y, q]
    origin = jnp.where(row8 == 0, gx, jnp.where(row8 == 1, gy * CY + CY // 2, gz * CZ)).astype(F32)
    origin = jnp.where(row8 < 3, origin, 0.0)
    scale = jnp.where(row8 < 3, SCALE, 1.0).astype(F32)
    for copy in halo:
        copy.wait()
    feature_windows(halo_ref, win_ref, origin, scale)
    compose(win_ref, tile_ref)
    exchange_wait(out_ref, in_ref, asend, arecv)
    decode(in_ref, meta_ref, metas_ref, local_sem.at[1])
    take_points(in_ref, metas_ref, turn_ref, origin, scale)

    first_pass(turn_ref, tile_ref, ahead_ref, late_ref, zp_ref, acc_ref)
    uncompose(acc_ref, wide_ref, 1)

    def fold(xy, carry):
        quads = fold_quads(wide_ref, xy, lane8)
        part_ref[xy] = jnp.concatenate([quad[0:1] for quad in quads] + [jnp.zeros((2, LANES), F32)], axis=0)
        return carry

    lax.fori_loop(0, COLUMNS, fold, 0)
    copies = near_copies(part_ref, box_ref, near_sem.at[2], near_sem.at[3])
    for copy in copies:
        copy.start()
    sums = [part_ref[ROWS + y + 1][1 : QUADS + 1] for y in range(CY)]
    for d, (ox, oy, oz) in enumerate(OFFSETS):
        copies[d].wait_recv()
        for k in range(CY if oy == 0 else 1):
            y = owner_row(oy, k)
            sums[y] = sums[y] + quads_of(box_ref[d, k], oz)
    for y in range(CY):
        opacity = jnp.concatenate([gauss_ref[y, q][3:4] for q in range(QUADS)], axis=0)
        valid = opacity > 0.0
        total_g = FLOOR + jnp.where(valid, sums[y] / jnp.where(valid, opacity, 1.0), 0.0)
        blank = jnp.zeros((8 - QUADS, LANES), F32)
        inv_ref[1, ROWS + y + 1] = jnp.concatenate([1.0 / total_g, blank], axis=0)
        loss = jnp.where(valid, -WIDTH * jnp.log(total_g), 0.0)
        loss_ref[y] = jnp.concatenate([loss, opacity], axis=0)
    back = inverse_copies(inv_ref, near_sem.at[4], near_sem.at[5])
    for copy in back:
        copy.start()
    for copy in copies:
        copy.wait_send()
    for copy in back:
        copy.wait()
    inverse_windows(inv_ref, win_ref)
    compose(win_ref, tile_ref)

    second_pass(turn_ref, tile_ref, ahead_ref, late_ref, zp_ref, acc_ref, stage_ref)
    answer_points(stage_ref, res_ref, metas_ref, reply_ref)
    exchange_start(reply_ref, ans_ref, bsend, brecv)
    ans_ref[me] = reply_ref[me]
    uncompose(acc_ref, wide_ref, 4)

    def fold_pull(xy, carry):
        quads = fold_quads(wide_ref, xy, lane8)
        for m in range(3):
            pull_ref[xy, m] = jnp.where(row8 < 4, quads[2 * m], quads[2 * m + 1])
        return carry

    lax.fori_loop(0, COLUMNS, fold_pull, 0)
    copies = near_copies(pull_ref, pulls_ref, near_sem.at[6], near_sem.at[7])
    for copy in copies:
        copy.start()
    sums = [[pull_ref[ROWS + y + 1, m] for m in range(3)] for y in range(CY)]
    for d, (ox, oy, oz) in enumerate(OFFSETS):
        copies[d].wait_recv()
        for k in range(CY if oy == 0 else 1):
            y = owner_row(oy, k)
            if oz == 0:
                for m in range(3):
                    sums[y][m] = sums[y][m] + pulls_ref[d, k, m]
            elif oz > 0:
                sums[y][0] = sums[y][0] + jnp.where(row8 >= 4, pulls_ref[d, k, 2], 0.0)
            else:
                sums[y][2] = sums[y][2] + jnp.where(row8 < 4, pulls_ref[d, k, 0], 0.0)
    for y in range(CY):
        for q in range(QUADS):
            m, half = divmod(q + 1, 2)
            tile = sums[y][m][4 * half : 4 * half + 4]
            loss = loss_ref[y][q : q + 1]
            opacity = loss_ref[y][QUADS + q : QUADS + q + 1]
            valid = opacity > 0.0
            dense = loss - WIDTH * (tile / jnp.where(valid, opacity, 1.0))
            tile = jnp.where(iota((4, LANES), 0) < 3, tile * (-BACK), dense)
            tile = jnp.where(valid, tile, 0.0)
            for r in range(4):
                grad_ref[0, y, 4 * q + r] = tile[:, SLOTS * r : SLOTS * r + SLOTS]
    for copy in copies:
        copy.wait_send()
    exchange_wait(reply_ref, ans_ref, bsend, brecv)

    def place(b, carry):
        cell = cell_ref[b]
        brick = ((cell >> 10 & 7) * SY + (cell >> 8 & 3)) * SZ + (cell >> 4 & 3)
        tile = ans_ref[brick]
        tile = jnp.where(homes_ref[0, brick] == b, tile, pltpu.roll(tile, 4, 0))
        point_ref[b] = tile[0:4]
        return carry

    lax.fori_loop(0, BLOCKS, place, 0)


def on_device(point_xyz, point_weight, block_cell, block_count, gauss_mean, gauss_opacity, gauss_count):
    dma = pltpu.SemaphoreType.DMA
    return pl.pallas_call(
        kernel,
        out_shape=(
            jax.ShapeDtypeStruct((BLOCKS, 4, LANES), F32),
            jax.ShapeDtypeStruct((1, CY, CZ, 4, SLOTS), F32),
        ),
        in_specs=[SMEM, SMEM, SMEM, VMEM, VMEM, VMEM, VMEM],
        out_specs=(VMEM, VMEM),
        scratch_shapes=[
            pltpu.VMEM((BLOCKS + 1, 8, LANES), F32),
            pltpu.VMEM((BRICKS, 8, LANES), F32),
            pltpu.VMEM((BRICKS, 8, LANES), F32),
            pltpu.VMEM((8, LANES), I32),
            pltpu.SMEM((8, LANES), I32),
            pltpu.VMEM((CY, QUADS, 8, LANES), F32),
            pltpu.VMEM((3, ROWS, QUADS + 2, 8, LANES), F32),
            pltpu.VMEM((CZ, COLUMNS, 8, LANES), F32),
            pltpu.VMEM((CELLS, TILES, 8, LANES), F32),
            pltpu.VMEM((CELLS + 8, LANES), I32),
            pltpu.SMEM((CELLS + 8, LANES), I32),
            pltpu.VMEM((CELLS, LANES, 8), F32),
            pltpu.VMEM((4 * GROUPS, 8, LANES), F32),
            pltpu.VMEM((4 * GROUPS, 8, LANES), F32),
            pltpu.VMEM((ITEMS * GROUPS, 8, LANES), F32),
            pltpu.VMEM((CELLS, 4 * TILES, 8, LANES), F32),
            pltpu.VMEM((CZ, COLUMNS, 8, LANES), F32),
            pltpu.VMEM((COLUMNS, 8, LANES), F32),
            pltpu.VMEM((26, CY, 8, LANES), F32),
            pltpu.VMEM((3, COLUMNS, 8, LANES), F32),
            pltpu.VMEM((CY, 8, LANES), F32),
            pltpu.VMEM((CELLS, LANES, 8), F32),
            pltpu.VMEM((CELLS, 8, LANES), F32),
            pltpu.VMEM((BRICKS, 8, LANES), F32),
            pltpu.VMEM((BRICKS, 8, LANES), F32),
            pltpu.VMEM((COLUMNS, 3, 8, LANES), F32),
            pltpu.VMEM((26, CY, 3, 8, LANES), F32),
            dma((2,)),
            dma((BRICKS,)),
            dma((BRICKS,)),
            dma((BRICKS,)),
            dma((BRICKS,)),
            dma((8, 26)),
        ],
        compiler_params=pltpu.CompilerParams(
            collective_id=0, has_side_effects=True, vmem_limit_bytes=56 * 1024 * 1024
        ),
        name="chamfer",
    )(block_cell, block_count, gauss_count, point_xyz, point_weight, gauss_mean, gauss_opacity)


def solution(mesh):
    return jax.shard_map(
        on_device,
        mesh=mesh,
        in_specs=(
            P(AXES, None, None),
            P(AXES, None),
            P(AXES),
            P(AXES),
            P("gx", "gy", "gz", None, None),
            P("gx", "gy", "gz", None),
            P("gx", "gy", "gz"),
        ),
        out_specs=(P(AXES, None, None), P("gx", "gy", "gz", None, None)),
        check_vma=False,
    )
```

```python
import functools
import math

import jax
import jax.numpy as jnp
from jax import lax
from jax.experimental import pallas as pl
from jax.experimental.pallas import tpu as pltpu
from jax.sharding import PartitionSpec as P

AXES = ("gx", "gy", "gz")
SX, SY, SZ = 8, 4, 4
BRICKS = SX * SY * SZ
CY, CZ = 4, 16
CELLS = CY * CZ
BLOCKS = 48
SLOTS = 32
LANES = 128
QUADS = CZ // 4
FIRST_GROUPS = 8
SECOND_GROUPS = 4
TILES = 7
ROWS = CY + 2
COLUMNS = 3 * ROWS

LOG2E = 1.4426950408889634
WIDTH = 0.05
CUTOFF = 0.5
SHARP = CUTOFF / WIDTH * LOG2E
LIFT = math.log2(SHARP)
SCALE = math.sqrt(LOG2E / CUTOFF)
BACK = 2.0 / (SHARP * SCALE)
FLOOR = math.exp(-10.0)
GONE = -1.0e4
NUDGE = 4.0e-6

F32 = jnp.float32
I32 = jnp.int32
VMEM = pl.BlockSpec(memory_space=pltpu.VMEM)
SMEM = pl.BlockSpec(memory_space=pltpu.SMEM)
MESH = pl.DeviceIdType.MESH


def iota(shape, dim):
    return lax.broadcasted_iota(I32, shape, dim)


def here():
    return lax.axis_index("gx"), lax.axis_index("gy"), lax.axis_index("gz")


def place_of(brick):
    return (brick // (SY * SZ), brick // SZ % SY, brick % SZ)


OFFSETS = [
    (ox, oy, oz)
    for ox in (-1, 0, 1)
    for oy in (-1, 0, 1)
    for oz in (-1, 0, 1)
    if (ox, oy, oz) != (0, 0, 0)
]
OFFSETS.sort(key=lambda o: abs(o[1]) + abs(o[2]))


def neighbour(offset):
    gx, gy, gz = here()
    ox, oy, oz = offset
    return ((gx + ox + SX) % SX, (gy + oy + SY) % SY, (gz + oz + SZ) % SZ)


def every_peer(act):
    gx, gy, gz = here()
    near = [((gy + dy) % SY, (gz + dz) % SZ) for dy in range(SY) for dz in range(SZ)]

    def plane(dx, first):
        px = (gx + dx) % SX
        for k in range(first, SY * SZ):
            py, pz = near[k]
            act(dx * (SY * SZ) + k, px * (SY * SZ) + (py * SZ + pz), (px, py, pz))

    def step(dx, carry):
        plane(dx, 0)
        return carry

    lax.fori_loop(1, SX, step, 0)
    plane(0, 1)


def exchange_copy(src_ref, dst_ref, send_sem, recv_sem, i, peer, device):
    gx, gy, gz = here()
    me = (gx * SY + gy) * SZ + gz
    return pltpu.make_async_remote_copy(
        src_ref=src_ref.at[peer],
        dst_ref=dst_ref.at[me],
        send_sem=send_sem.at[i],
        recv_sem=recv_sem.at[i],
        device_id=device,
        device_id_type=MESH,
    )


def exchange_start(*refs):
    every_peer(lambda i, peer, device: exchange_copy(*refs, i, peer, device).start())


def exchange_wait(*refs):
    every_peer(lambda i, peer, device: exchange_copy(*refs, i, peer, device).wait())


def spread(row):
    return jnp.broadcast_to(row, (8, LANES))


def signal_all():
    barrier = pltpu.get_barrier_semaphore()
    every_peer(
        lambda i, peer, device: pl.semaphore_signal(barrier, inc=1, device_id=device, device_id_type=MESH)
    )


def pack_points(cell_ref, count_ref, xyz_ref, weight_ref, pay_ref, out_ref, home_ref, homes_ref, sem):
    lane = iota((1, LANES), 1)
    row4 = iota((4, LANES), 0)
    lane4 = iota((4, LANES), 1)
    row8 = iota((8, LANES), 0)

    def payload(b, carry):
        first, second = carry
        cell = cell_ref[b]
        cx = cell >> 10 & 7
        cy = (cell >> 6) & 15
        cz = cell & 63
        brick = (cx * SY + (cy >> 2)) * SZ + (cz >> 4)
        hit = lane == brick
        later = hit & (first < BLOCKS)
        second = jnp.where(later, b, second)
        first = jnp.where(hit & (first == BLOCKS), b, first)
        weight = jnp.where(lane < count_ref[b], weight_ref[pl.ds(b, 1), :], 0.0)
        rows = jnp.concatenate([xyz_ref[k, pl.ds(b, 1), :] for k in range(3)] + [weight], axis=0)
        corner = jnp.where(row4 == 0, cx, jnp.where(row4 == 1, cy, cz))
        top = (corner + 1).astype(F32) - NUDGE
        rows = jnp.where((lane4 == 0) & (row4 < 3), jnp.minimum(rows, top), rows)
        pay_ref[b] = jnp.concatenate([rows, rows], axis=0)
        return first, second

    none = jnp.full((1, LANES), BLOCKS, I32)
    first, second = lax.fori_loop(0, BLOCKS, payload, (none, none))
    pay_ref[BLOCKS] = jnp.zeros((8, LANES), F32)
    home_ref[...] = jnp.where(row8 == 0, first, second)
    copy = pltpu.make_async_copy(home_ref, homes_ref, sem)
    copy.start()
    copy.wait()

    def put(i, carry):
        for u in range(4):
            d = i * 4 + u
            first = jnp.clip(homes_ref[0, d], 0, BLOCKS)
            second = jnp.clip(homes_ref[1, d], 0, BLOCKS)
            out_ref[d] = jnp.where(row8 < 4, pay_ref[first], pay_ref[second])
        return carry

    lax.fori_loop(0, BRICKS // 4, put, 0)


def pack_gauss(gcount_ref, mean_ref, opacity_ref, gauss_ref):
    lane = iota((1, LANES), 1)
    for y in range(CY):
        for q in range(QUADS):
            mean = jnp.concatenate([mean_ref[0, y, :, 4 * q + r, :] for r in range(4)], axis=1)
            opacity = jnp.concatenate(
                [opacity_ref[0, y, 4 * q + r : 4 * q + r + 1, :] for r in range(4)], axis=1
            )
            have = [gcount_ref[0, y, 4 * q + r] for r in range(4)]
            count = jnp.where(
                lane < 64,
                jnp.where(lane < 32, have[0], have[1]),
                jnp.where(lane < 96, have[2], have[3]),
            )
            opacity = jnp.where((lane & 31) < count, opacity, 0.0)
            gauss_ref[y, q] = jnp.concatenate([mean, opacity, jnp.zeros((4, LANES), F32)], axis=0)


def side(o, last):
    if o == 0:
        return 0, 1, last + 1
    return (last, 0, 1) if o > 0 else (0, last + 2, 1)


def halo_copies(gauss_ref, halo_ref, send_sem, recv_sem):
    copies = []
    for d, (ox, oy, oz) in enumerate(OFFSETS):
        sy, ty, ny = side(oy, CY - 1)
        sq, tq, nq = side(oz, QUADS - 1)
        copies.append(
            pltpu.make_async_remote_copy(
                src_ref=gauss_ref.at[pl.ds(sy, ny), pl.ds(sq, nq), pl.ds(0, 4)],
                dst_ref=halo_ref.at[1 - ox, pl.ds(ty, ny), pl.ds(tq, nq), pl.ds(0, 4)],
                send_sem=send_sem.at[d],
                recv_sem=recv_sem.at[d],
                device_id=neighbour((ox, oy, oz)),
                device_id_type=MESH,
            )
        )
    return copies


def near_copies(part_ref, box_ref, send_sem, recv_sem):
    copies = []
    for d, (ox, oy, oz) in enumerate(OFFSETS):
        y0, ny = (1, CY) if oy == 0 else ((CY + 1, 1) if oy > 0 else (0, 1))
        copies.append(
            pltpu.make_async_remote_copy(
                src_ref=part_ref.at[pl.ds((1 + ox) * ROWS + y0, ny)],
                dst_ref=box_ref.at[d, pl.ds(0, ny)],
                send_sem=send_sem.at[d],
                recv_sem=recv_sem.at[d],
                device_id=neighbour((ox, oy, oz)),
                device_id_type=MESH,
            )
        )
    return copies


def pull_copies(pull_ref, box_ref, send_sem, recv_sem):
    copies = []
    for d, (ox, oy, oz) in enumerate(OFFSETS):
        y0, ny = (1, CY) if oy == 0 else ((CY + 1, 1) if oy > 0 else (0, 1))
        m0, nm = (0, 2) if oz == 0 else (2, 1)
        copies.append(
            pltpu.make_async_remote_copy(
                src_ref=pull_ref.at[pl.ds(m0, nm), pl.ds((1 + ox) * ROWS + y0, ny)],
                dst_ref=box_ref.at[d, pl.ds(0, nm), pl.ds(0, ny)],
                send_sem=send_sem.at[d],
                recv_sem=recv_sem.at[d],
                device_id=neighbour((ox, oy, oz)),
                device_id_type=MESH,
            )
        )
    return copies


def inverse_copies(inv_ref, send_sem, recv_sem):
    copies = []
    for d, (ox, oy, oz) in enumerate(OFFSETS):
        sy, ty, ny = side(oy, CY - 1)
        copies.append(
            pltpu.make_async_remote_copy(
                src_ref=inv_ref.at[1, pl.ds(ROWS + 1 + sy, ny)],
                dst_ref=inv_ref.at[1 - oz, pl.ds((1 - ox) * ROWS + ty, ny)],
                send_sem=send_sem.at[d],
                recv_sem=recv_sem.at[d],
                device_id=neighbour((ox, oy, oz)),
                device_id_type=MESH,
            )
        )
    return copies


def feature_windows(halo_ref, win_ref, origin, scale):
    gx, gy, gz = here()
    row8 = iota((8, LANES), 0)
    lane8 = iota((8, LANES), 1)

    def windows(y, carry):
        for x in range(3):
            window(x, y)
        return carry

    def window(x, y):
        xy = x * ROWS + y
        outside = ((x == 0) & (gx == 0)) | ((x == 2) & (gx == SX - 1))
        outside = outside | ((y == 0) & (gy == 0)) | ((y == CY + 1) & (gy == SY - 1))
        tiles = []
        for q in range(QUADS + 2):
            gone = outside
            if q == 0:
                gone = gone | (gz == 0)
            if q == QUADS + 1:
                gone = gone | (gz == SZ - 1)
            tile = halo_ref[x, y, q]
            opacity = jnp.where(gone, 0.0, tile)
            strength = jnp.where(opacity > 0.0, jnp.log2(jnp.maximum(opacity, 1e-30)) - SHARP, GONE)
            tiles.append(jnp.where(row8 == 3, strength, (tile - origin) * scale))
        for z in range(CZ):
            a, b = z // 4, z % 4
            if b == 0:
                tile = pltpu.roll(jnp.where(lane8 >= 96, tiles[a], tiles[a + 1]), 32, 1)
            elif b == 1:
                tile = tiles[a + 1]
            elif b == 2:
                tile = pltpu.roll(tiles[a + 1], 96, 1)
            else:
                tile = pltpu.roll(jnp.where(lane8 < 64, tiles[a + 2], tiles[a + 1]), 64, 1)
            tile = jnp.where((row8 == 3) & (lane8 >= 96), GONE, tile)
            win_ref[z, xy] = jnp.where(row8 == 2, tile - z * SCALE, tile)

    lax.fori_loop(0, ROWS, windows, 0)


def inverse_windows(inv_ref, win_ref):
    row8 = iota((8, LANES), 0)
    lane1 = iota((1, LANES), 1)

    def windows(y, carry):
        for x in range(3):
            window(x * ROWS + y)
        return carry

    def window(xy):
        own = inv_ref[1, xy]
        rows = [inv_ref[0, xy][QUADS - 1 : QUADS]] + [own[q : q + 1] for q in range(QUADS)]
        tile = jnp.concatenate(rows + [inv_ref[2, xy][0:1], jnp.zeros((2, LANES), F32)], axis=0)
        moved = [pltpu.roll(tile, 32, 1), tile, pltpu.roll(tile, 96, 1), pltpu.roll(tile, 64, 1)]
        for z in range(CZ):
            a, b = z // 4, z % 4
            row = moved[b][a + 1 : a + 2]
            if b == 0:
                row = jnp.where(lane1 < 32, moved[b][a : a + 1], row)
            elif b == 3:
                row = jnp.where(lane1 >= 64, moved[b][a + 2 : a + 3], row)
            win_ref[z, xy] = jnp.where(row8 == 4, row, win_ref[z, xy])

    lax.fori_loop(0, ROWS, windows, 0)


TRIPLES = [(x, dy, divmod(3 * (3 * x + dy), 4)) for x in range(3) for dy in range(3)]


def compose(win_ref, tile_ref):
    lane8 = iota((8, LANES), 1)

    def one(z, carry):
        for y in range(CY):
            tiles = [None] * (TILES + 1)
            for x, dy, (j, p) in TRIPLES:
                piece = win_ref[z, x * ROWS + y + dy]
                if p:
                    piece = pltpu.roll(piece, 32 * p, 1)
                    tiles[j] = jnp.where(lane8 < 32 * p, tiles[j], piece)
                else:
                    tiles[j] = piece
                tiles[j + 1] = piece
            for j in range(TILES):
                tile_ref[y * CZ + z, j] = tiles[j]
        return carry

    lax.fori_loop(0, CZ, one, 0)


def uncompose(acc_ref, wide_ref, count):
    row8 = iota((8, LANES), 0)
    lane8 = iota((8, LANES), 1)

    def one(z, carry):
        wide = [None] * COLUMNS
        for y in range(CY):
            tiles = []
            for j in range(TILES):
                at = y * CZ + z
                rows = [jnp.sum(acc_ref[at, j * count + k], axis=0, keepdims=True) for k in range(count)]
                tile = spread(rows[0])
                for k in range(1, count):
                    tile = jnp.where((row8 & 3) == k, rows[k], tile)
                tiles.append(tile)
            for x, dy, (j, p) in TRIPLES:
                tile = tiles[j]
                if p:
                    tile = pltpu.roll(jnp.where(lane8 >= 32 * p, tiles[j], tiles[j + 1]), LANES - 32 * p, 1)
                at = x * ROWS + y + dy
                wide[at] = tile if wide[at] is None else wide[at] + tile
        for at in range(COLUMNS):
            wide_ref[z, at] = jnp.where(lane8 < 96, wide[at], 0.0)
        return carry

    lax.fori_loop(0, CZ, one, 0)


def clear(acc_ref):
    def one(c, carry):
        for j in range(4 * TILES):
            acc_ref[c, j] = jnp.zeros((8, LANES), F32)
        return carry

    lax.fori_loop(0, CELLS, one, 0)


def fold_quads(wide_ref, xy, lane8):
    quads = [jnp.zeros((8, LANES), F32) for q in range(QUADS + 2)]
    for z in range(CZ):
        tile = wide_ref[z, xy]
        a, b = z // 4, z % 4
        if b == 1:
            quads[a + 1] = quads[a + 1] + tile
        elif b == 2:
            quads[a + 1] = quads[a + 1] + pltpu.roll(tile, 32, 1)
        elif b == 0:
            moved = pltpu.roll(tile, 96, 1)
            quads[a] = quads[a] + jnp.where(lane8 >= 96, moved, 0.0)
            quads[a + 1] = quads[a + 1] + jnp.where(lane8 < 96, moved, 0.0)
        else:
            moved = pltpu.roll(tile, 64, 1)
            quads[a + 1] = quads[a + 1] + jnp.where(lane8 >= 64, moved, 0.0)
            quads[a + 2] = quads[a + 2] + jnp.where(lane8 < 64, moved, 0.0)
    return quads


def decode(in_ref, meta_ref, metas_ref, sem):
    gx, gy, gz = here()
    row8 = iota((8, LANES), 0)
    lane8 = iota((8, LANES), 1)

    def gather(i, found):
        for u in range(32):
            s = i * 32 + u
            found = jnp.where(lane8 == s, jnp.broadcast_to(in_ref[s][:, 0:1], (8, LANES)), found)
        return found

    found = lax.fori_loop(0, BRICKS // 32, gather, jnp.zeros((8, LANES), F32))
    cell = iota((CELLS, LANES), 0).astype(F32)
    lane64 = iota((CELLS, LANES), 1).astype(F32)
    slot = jnp.full((CELLS, LANES), -1.0, F32)
    labels = []
    for k in range(2):
        y0 = jnp.floor(found[4 * k + 1 : 4 * k + 2]) - (gy * CY).astype(F32)
        z0 = jnp.floor(found[4 * k + 2 : 4 * k + 3]) - (gz * CZ).astype(F32)
        label = jnp.where(found[4 * k + 3 : 4 * k + 4] > 0.0, y0 * CZ + z0, -1.0)
        slot = jnp.where(label == cell, 2.0 * lane64 + k, slot)
        labels.append(jnp.clip(label, 0.0, CELLS - 1.0))
    slot = jnp.max(slot, axis=1, keepdims=True)
    meta_ref[pl.ds(0, CELLS), :] = jnp.broadcast_to(slot, (CELLS, LANES)).astype(I32)
    meta_ref[pl.ds(CELLS, 8), :] = jnp.where(row8 == 0, labels[0], labels[1]).astype(I32)
    copy = pltpu.make_async_copy(meta_ref, metas_ref, sem)
    copy.start()
    copy.wait()


def take_points(in_ref, metas_ref, pts_ref, origin, scale):
    row8 = iota((8, LANES), 0)

    def prepare(i, carry):
        for u in range(8):
            c = i * 8 + u
            slot = metas_ref[c, 0]
            safe = jnp.clip(slot, 0, 2 * BRICKS - 1)
            tile = in_ref[safe >> 1]
            tile = jnp.where((safe & 1) == 1, pltpu.roll(tile, 4, 0), tile)
            tile = jnp.where(slot >= 0, tile, 0.0)
            shift = origin + jnp.where(row8 == 2, (c % CZ).astype(F32), 0.0)
            weight = jnp.where(tile > 0.0, jnp.log2(jnp.maximum(tile, 1e-30)), GONE)
            pts_ref[c] = jnp.where(row8 == 3, weight, (tile - shift) * scale)
        return carry

    lax.fori_loop(0, CELLS // 8, prepare, 0)
    pts_ref[CELLS] = jnp.zeros((8, LANES), F32)


def rows_of(i, groups):
    chunks = LANES // (8 * groups)
    return i // chunks, i % chunks * (8 * groups)


def turn(pts_ref, feat_ref, c, f):
    row = jnp.broadcast_to(pts_ref[c, pl.ds(f, 1), :], (LANES, LANES))
    feat_ref[f, pl.ds(c * 16, 16)] = jnp.transpose(row).reshape(16, 8, LANES)


def first_pass(pts_ref, feat_ref, tile_ref, late_ref, zp_ref, acc_ref):
    groups = FIRST_GROUPS
    items = CELLS * LANES // (8 * groups)
    for f in range(4):
        turn(pts_ref, feat_ref, 0, f)
    for g in range(groups):
        late_ref[g] = jnp.zeros((8, LANES), F32)

    def settle(i):
        for g in range(groups):
            total = jnp.sum(late_ref[g], axis=1, keepdims=True)
            zp_ref[i * groups + g] = jnp.broadcast_to(total, (8, LANES))

    def sweep(i, carry):
        feats = [[feat_ref[f, i * groups + g] for f in range(4)] for g in range(groups)]
        settle((i + items - 1) % items)
        for f in range(2):
            turn(pts_ref, feat_ref, i // 2 + 1, i % 2 * 2 + f)
        c, first = rows_of(i, groups)
        sums = [None] * groups
        for j in range(TILES):
            mx, my, mz, la = [spread(tile_ref[c, j, f : f + 1, :]) for f in range(4)]
            far = None
            for g in range(groups):
                px, py, pz, lw = feats[g]
                ex, ey, ez = px - mx, py - my, pz - mz
                fall = jnp.exp2(LIFT - ex * ex - ey * ey - ez * ez)
                term = jnp.exp2(fall + (la + lw))
                sums[g] = term if sums[g] is None else sums[g] + term
                far = term if far is None else far + term
            acc_ref[c, j] = acc_ref[c, j] + far
        for g in range(groups):
            late_ref[g] = sums[g]
        return carry

    lax.fori_loop(0, items, sweep, 0)
    settle(items - 1)


def second_pass(feat_ref, tile_ref, late_ref, zp_ref, acc_ref, stage_ref):
    groups = SECOND_GROUPS
    items = CELLS * LANES // (8 * groups)
    for g in range(4 * groups):
        late_ref[g] = jnp.ones((8, LANES), F32)
    lane = iota((8, LANES), 1) & 3

    def settle(i):
        c, first = rows_of(i, groups)
        for g in range(groups):
            out = (WIDTH * jnp.log(late_ref[4 * g + 3]))
            for k in range(3):
                total = jnp.sum(late_ref[4 * g + k], axis=1, keepdims=True) * BACK
                out = jnp.where(lane == k + 1, total, out)
            stage_ref[c, pl.ds(pl.multiple_of(first + 8 * g, 8), 8), :] = out[:, 0:8]

    def sweep(i, carry):
        feats = [[feat_ref[f, i * groups + g] for f in range(4)] for g in range(groups)]
        settle((i + items - 1) % items)
        c, first = rows_of(i, groups)
        inverse = []
        for g in range(groups):
            lw = feats[g][3]
            total = FLOOR + zp_ref[i * groups + g] * jnp.exp2(-jnp.maximum(lw, -64.0))
            inverse.append(jnp.where(lw > 0.5 * GONE, 1.0 / total, 1.0))
        sums = [[None] * 3 for g in range(groups)]
        for j in range(TILES):
            mx, my, mz, la, ig = [spread(tile_ref[c, j, f : f + 1, :]) for f in range(5)]
            far = [None] * 4
            for g in range(groups):
                px, py, pz, lw = feats[g]
                ex, ey, ez = px - mx, py - my, pz - mz
                fall = jnp.exp2(LIFT - ex * ex - ey * ey - ez * ez)
                term = jnp.exp2(fall + (la + lw))
                pull = (term * fall) * (inverse[g] + ig)
                parts = [pull * ex, pull * ey, pull * ez, term * inverse[g]]
                sums[g] = [p if s is None else s + p for s, p in zip(sums[g], parts)]
                far = [p if s is None else s + p for s, p in zip(far, parts)]
            for k in range(4):
                acc_ref[c, 4 * j + k] = acc_ref[c, 4 * j + k] + far[k]
        for g in range(groups):
            for k in range(3):
                late_ref[4 * g + k] = sums[g][k]
            late_ref[4 * g + 3] = inverse[g]
        return carry

    lax.fori_loop(0, items, sweep, 0)
    settle(items - 1)


def answer_points(stage_ref, res_ref, metas_ref, reply_ref):
    row8 = iota((8, LANES), 0)

    def turn(i, carry):
        for u in range(8):
            res_ref[i * 8 + u] = jnp.transpose(stage_ref[i * 8 + u])
        return carry

    lax.fori_loop(0, CELLS // 8, turn, 0)

    def put(i, carry):
        for u in range(4):
            s = i * 4 + u
            first = jnp.clip(metas_ref[CELLS, s], 0, CELLS - 1)
            second = jnp.clip(metas_ref[CELLS + 1, s], 0, CELLS - 1)
            reply_ref[s] = jnp.where(row8 < 4, res_ref[first], res_ref[second])
        return carry

    lax.fori_loop(0, BRICKS // 4, put, 0)


def quads_of(tile, oz):
    if oz == 0:
        return tile[1 : QUADS + 1]
    row = iota((QUADS, LANES), 0)
    if oz > 0:
        return jnp.where(row == 0, tile[QUADS + 1 : QUADS + 2], 0.0)
    return jnp.where(row == QUADS - 1, tile[0:1], 0.0)


def owner_row(oy, k):
    return k if oy == 0 else (0 if oy > 0 else CY - 1)


def kernel(cell_ref, count_ref, gcount_ref, xyz_ref, weight_ref, mean_ref, opacity_ref,
           point_ref, grad_ref,
           pay_ref, out_ref, in_ref, home_ref, homes_ref, gauss_ref, halo_ref, win_ref, tile_ref,
           meta_ref, metas_ref, pts_ref, feat_ref, late_ref, zp_ref, acc_ref, wide_ref, part_ref,
           box_ref, inv_ref, loss_ref, stage_ref, res_ref, reply_ref, ans_ref, pull_ref, pulls_ref,
           local_sem, asend, arecv, bsend, brecv, near_sem):
    gx, gy, gz = here()
    me = (gx * SY + gy) * SZ + gz
    row8 = iota((8, LANES), 0)
    lane8 = iota((8, LANES), 1)
    signal_all()
    pack_gauss(gcount_ref, mean_ref, opacity_ref, gauss_ref)
    pack_points(cell_ref, count_ref, xyz_ref, weight_ref, pay_ref, out_ref, home_ref, homes_ref, local_sem.at[0])
    pl.semaphore_wait(pltpu.get_barrier_semaphore(), BRICKS - 1)
    halo = halo_copies(gauss_ref, halo_ref, near_sem.at[0], near_sem.at[1])
    for copy in halo:
        copy.start()
    exchange_start(out_ref, in_ref, asend, arecv)
    in_ref[me] = out_ref[me]
    for y in range(CY):
        for q in range(QUADS):
            halo_ref[1, y + 1, q + 1] = gauss_ref[y, q]
    origin = jnp.where(row8 == 0, gx, jnp.where(row8 == 1, gy * CY + CY // 2, gz * CZ)).astype(F32)
    origin = jnp.where(row8 < 3, origin, 0.0)
    scale = jnp.where(row8 < 3, SCALE, 1.0).astype(F32)
    for copy in halo:
        copy.wait()
    feature_windows(halo_ref, win_ref, origin, scale)
    compose(win_ref, tile_ref)
    clear(acc_ref)
    exchange_wait(out_ref, in_ref, asend, arecv)
    decode(in_ref, meta_ref, metas_ref, local_sem.at[1])
    take_points(in_ref, metas_ref, pts_ref, origin, scale)

    first_pass(pts_ref, feat_ref, tile_ref, late_ref, zp_ref, acc_ref)
    uncompose(acc_ref, wide_ref, 1)

    def fold(y, carry):
        for x in range(3):
            quads = fold_quads(wide_ref, x * ROWS + y, lane8)
            rows = [quad[0:1] for quad in quads] + [jnp.zeros((2, LANES), F32)]
            part_ref[x * ROWS + y] = jnp.concatenate(rows, axis=0)
        return carry

    lax.fori_loop(0, ROWS, fold, 0)
    copies = near_copies(part_ref, box_ref, near_sem.at[2], near_sem.at[3])
    for copy in copies:
        copy.start()
    clear(acc_ref)
    sums = [part_ref[ROWS + y + 1][1 : QUADS + 1] for y in range(CY)]
    for d, (ox, oy, oz) in enumerate(OFFSETS):
        copies[d].wait_recv()
        for k in range(CY if oy == 0 else 1):
            y = owner_row(oy, k)
            sums[y] = sums[y] + quads_of(box_ref[d, k], oz)
    for y in range(CY):
        opacity = jnp.concatenate([gauss_ref[y, q][3:4] for q in range(QUADS)], axis=0)
        valid = opacity > 0.0
        total_g = FLOOR + jnp.where(valid, sums[y] / jnp.where(valid, opacity, 1.0), 0.0)
        blank = jnp.zeros((8 - QUADS, LANES), F32)
        inv_ref[1, ROWS + y + 1] = jnp.concatenate([1.0 / total_g, blank], axis=0)
        loss = jnp.where(valid, -WIDTH * jnp.log(total_g), 0.0)
        loss_ref[y] = jnp.concatenate([loss, opacity], axis=0)
    back = inverse_copies(inv_ref, near_sem.at[4], near_sem.at[5])
    for copy in back:
        copy.start()
    for copy in copies:
        copy.wait_send()
    for copy in back:
        copy.wait()
    inverse_windows(inv_ref, win_ref)
    compose(win_ref, tile_ref)

    second_pass(feat_ref, tile_ref, late_ref, zp_ref, acc_ref, stage_ref)
    answer_points(stage_ref, res_ref, metas_ref, reply_ref)
    exchange_start(reply_ref, ans_ref, bsend, brecv)
    ans_ref[me] = reply_ref[me]
    uncompose(acc_ref, wide_ref, 4)

    def fold_pull(y, carry):
        for x in range(3):
            quads = fold_quads(wide_ref, x * ROWS + y, lane8)
            for m, (low, high) in enumerate(((1, 2), (3, 4), (0, 5))):
                pull_ref[m, x * ROWS + y] = jnp.where(row8 < 4, quads[low], quads[high])
        return carry

    lax.fori_loop(0, ROWS, fold_pull, 0)
    copies = pull_copies(pull_ref, pulls_ref, near_sem.at[6], near_sem.at[7])
    for copy in copies:
        copy.start()
    sums = [[pull_ref[m, ROWS + y + 1] for m in range(2)] for y in range(CY)]
    for d, (ox, oy, oz) in enumerate(OFFSETS):
        copies[d].wait_recv()
        for k in range(CY if oy == 0 else 1):
            y = owner_row(oy, k)
            if oz == 0:
                for m in range(2):
                    sums[y][m] = sums[y][m] + pulls_ref[d, m, k]
            elif oz > 0:
                outer = pltpu.roll(pulls_ref[d, 0, k], 4, 0)
                sums[y][0] = sums[y][0] + jnp.where(row8 < 4, outer, 0.0)
            else:
                outer = pltpu.roll(pulls_ref[d, 0, k], 4, 0)
                sums[y][1] = sums[y][1] + jnp.where(row8 >= 4, outer, 0.0)
    for y in range(CY):
        for q in range(QUADS):
            m, half = divmod(q, 2)
            tile = sums[y][m][4 * half : 4 * half + 4]
            loss = loss_ref[y][q : q + 1]
            opacity = loss_ref[y][QUADS + q : QUADS + q + 1]
            valid = opacity > 0.0
            dense = loss - WIDTH * (tile / jnp.where(valid, opacity, 1.0))
            tile = jnp.where(iota((4, LANES), 0) < 3, tile * (-BACK), dense)
            tile = jnp.where(valid, tile, 0.0)
            parts = [tile[:, SLOTS * r : SLOTS * r + SLOTS] for r in range(4)]
            for r in (0, 2):
                both = jnp.concatenate(parts[r : r + 2], axis=0)
                grad_ref[pl.ds(4 * (y * CZ + 4 * q + r), 8), :] = both
    for copy in copies:
        copy.wait_send()
    exchange_wait(reply_ref, ans_ref, bsend, brecv)

    def place(i, carry):
        for u in range(4):
            tiles = []
            for k in range(2):
                b = i * 8 + u * 2 + k
                cell = cell_ref[b]
                brick = ((cell >> 10 & 7) * SY + (cell >> 8 & 3)) * SZ + (cell >> 4 & 3)
                tile = ans_ref[brick]
                half = (homes_ref[0, brick] != b).astype(I32)
                tiles.append(jnp.where(half == k, tile, pltpu.roll(tile, 4, 0)))
            point_ref[pl.ds(pl.multiple_of(i * 32 + u * 8, 8), 8), :] = jnp.where(row8 < 4, tiles[0], tiles[1])
        return carry

    lax.fori_loop(0, BLOCKS // 8, place, 0)


def on_device(point_xyz, point_weight, block_cell, block_count, gauss_mean, gauss_opacity, gauss_count):
    dma = pltpu.SemaphoreType.DMA
    point_out, gauss_grad = pl.pallas_call(
        kernel,
        out_shape=(
            jax.ShapeDtypeStruct((BLOCKS * 4, LANES), F32),
            jax.ShapeDtypeStruct((CELLS * 4, SLOTS), F32),
        ),
        in_specs=[SMEM, SMEM, SMEM, VMEM, VMEM, VMEM, VMEM],
        out_specs=(VMEM, VMEM),
        scratch_shapes=[
            pltpu.VMEM((BLOCKS + 1, 8, LANES), F32),
            pltpu.VMEM((BRICKS, 8, LANES), F32),
            pltpu.VMEM((BRICKS, 8, LANES), F32),
            pltpu.VMEM((8, LANES), I32),
            pltpu.SMEM((8, LANES), I32),
            pltpu.VMEM((CY, QUADS, 8, LANES), F32),
            pltpu.VMEM((3, ROWS, QUADS + 2, 8, LANES), F32),
            pltpu.VMEM((CZ, COLUMNS, 8, LANES), F32),
            pltpu.VMEM((CELLS, TILES, 8, LANES), F32),
            pltpu.VMEM((CELLS + 8, LANES), I32),
            pltpu.SMEM((CELLS + 8, LANES), I32),
            pltpu.VMEM((CELLS + 1, 8, LANES), F32),
            pltpu.VMEM((4, (CELLS + 1) * 16, 8, LANES), F32),
            pltpu.VMEM((4 * SECOND_GROUPS, 8, LANES), F32),
            pltpu.VMEM((CELLS * 16, 8, LANES), F32),
            pltpu.VMEM((CELLS, 4 * TILES, 8, LANES), F32),
            pltpu.VMEM((CZ, COLUMNS, 8, LANES), F32),
            pltpu.VMEM((COLUMNS, 8, LANES), F32),
            pltpu.VMEM((26, CY, 8, LANES), F32),
            pltpu.VMEM((3, COLUMNS, 8, LANES), F32),
            pltpu.VMEM((CY, 8, LANES), F32),
            pltpu.VMEM((CELLS, LANES, 8), F32),
            pltpu.VMEM((CELLS, 8, LANES), F32),
            pltpu.VMEM((BRICKS, 8, LANES), F32),
            pltpu.VMEM((BRICKS, 8, LANES), F32),
            pltpu.VMEM((3, COLUMNS, 8, LANES), F32),
            pltpu.VMEM((26, 2, CY, 8, LANES), F32),
            dma((2,)),
            dma((BRICKS,)),
            dma((BRICKS,)),
            dma((BRICKS,)),
            dma((BRICKS,)),
            dma((8, 26)),
        ],
        compiler_params=pltpu.CompilerParams(
            collective_id=0, has_side_effects=True, vmem_limit_bytes=56 * 1024 * 1024
        ),
        name="chamfer",
    )(
        block_cell,
        block_count,
        gauss_count,
        point_xyz.transpose(1, 0, 2),
        point_weight,
        gauss_mean.transpose(0, 1, 3, 2, 4),
        gauss_opacity,
    )
    return point_out.reshape(BLOCKS, 4, LANES), gauss_grad.reshape(1, CY, CZ, 4, SLOTS)


def solution(mesh):
    return jax.shard_map(
        on_device,
        mesh=mesh,
        in_specs=(
            P(AXES, None, None),
            P(AXES, None),
            P(AXES),
            P(AXES),
            P("gx", "gy", "gz", None, None),
            P("gx", "gy", "gz", None),
            P("gx", "gy", "gz"),
        ),
        out_specs=(P(AXES, None, None), P("gx", "gy", "gz", None, None)),
        check_vma=False,
    )
```

```python
import functools
import math

import jax
import jax.numpy as jnp
from jax import lax
from jax.experimental import pallas as pl
from jax.experimental.pallas import tpu as pltpu
from jax.sharding import PartitionSpec as P

AXES = ("gx", "gy", "gz")
SX, SY, SZ = 8, 4, 4
BRICKS = SX * SY * SZ
CY, CZ = 4, 16
CELLS = CY * CZ
BLOCKS = 48
SLOTS = 32
LANES = 128
QUADS = CZ // 4
GROUPS = 16
HALF = 8
PART = 8
FEATURE = (CELLS + 1) * GROUPS
TILES = 7
ROWS = CY + 2
COLUMNS = 3 * ROWS

LOG2E = 1.4426950408889634
WIDTH = 0.05
CUTOFF = 0.5
SHARP = CUTOFF / WIDTH * LOG2E
LIFT = math.log2(SHARP)
SCALE = math.sqrt(LOG2E / CUTOFF)
BACK = 2.0 / (SHARP * SCALE)
FLOOR = math.exp(-10.0)
GONE = -1.0e4
NUDGE = 4.0e-6

F32 = jnp.float32
I32 = jnp.int32
VMEM = pl.BlockSpec(memory_space=pltpu.VMEM)
SMEM = pl.BlockSpec(memory_space=pltpu.SMEM)
MESH = pl.DeviceIdType.MESH


def iota(shape, dim):
    return lax.broadcasted_iota(I32, shape, dim)


def here():
    return lax.axis_index("gx"), lax.axis_index("gy"), lax.axis_index("gz")


def place_of(brick):
    return (brick // (SY * SZ), brick // SZ % SY, brick % SZ)


OFFSETS = [
    (ox, oy, oz)
    for ox in (-1, 0, 1)
    for oy in (-1, 0, 1)
    for oz in (-1, 0, 1)
    if (ox, oy, oz) != (0, 0, 0)
]
OFFSETS.sort(key=lambda o: abs(o[1]) + abs(o[2]))


def neighbour(offset):
    gx, gy, gz = here()
    ox, oy, oz = offset
    return ((gx + ox + SX) % SX, (gy + oy + SY) % SY, (gz + oz + SZ) % SZ)


def every_peer(act):
    gx, gy, gz = here()
    near = [((gy + dy) % SY, (gz + dz) % SZ) for dy in range(SY) for dz in range(SZ)]

    def plane(dx, first):
        px = (gx + dx) % SX
        for k in range(first, SY * SZ):
            py, pz = near[k]
            act(dx * (SY * SZ) + k, px * (SY * SZ) + (py * SZ + pz), (px, py, pz))

    def step(dx, carry):
        plane(dx, 0)
        return carry

    lax.fori_loop(1, SX, step, 0)
    plane(0, 1)


def exchange_copy(src_ref, dst_ref, send_sem, recv_sem, i, peer, device):
    gx, gy, gz = here()
    me = (gx * SY + gy) * SZ + gz
    return pltpu.make_async_remote_copy(
        src_ref=src_ref.at[peer],
        dst_ref=dst_ref.at[me],
        send_sem=send_sem.at[i],
        recv_sem=recv_sem.at[i],
        device_id=device,
        device_id_type=MESH,
    )


def exchange_start(*refs):
    every_peer(lambda i, peer, device: exchange_copy(*refs, i, peer, device).start())


def exchange_wait(*refs):
    every_peer(lambda i, peer, device: exchange_copy(*refs, i, peer, device).wait())


def spread(row):
    return jnp.broadcast_to(row, (8, LANES))


def signal_all():
    barrier = pltpu.get_barrier_semaphore()
    every_peer(
        lambda i, peer, device: pl.semaphore_signal(barrier, inc=1, device_id=device, device_id_type=MESH)
    )


def pack_points(cell_ref, count_ref, xyz_ref, weight_ref, pay_ref, out_ref, home_ref, homes_ref, sem):
    lane = iota((1, LANES), 1)
    row4 = iota((4, LANES), 0)
    lane4 = iota((4, LANES), 1)
    row8 = iota((8, LANES), 0)

    def payload(b, carry):
        first, second = carry
        cell = cell_ref[b]
        cx = cell >> 10 & 7
        cy = (cell >> 6) & 15
        cz = cell & 63
        brick = (cx * SY + (cy >> 2)) * SZ + (cz >> 4)
        hit = lane == brick
        later = hit & (first < BLOCKS)
        second = jnp.where(later, b, second)
        first = jnp.where(hit & (first == BLOCKS), b, first)
        weight = jnp.where(lane < count_ref[b], weight_ref[pl.ds(b, 1), :], 0.0)
        rows = jnp.concatenate([xyz_ref[k, pl.ds(b, 1), :] for k in range(3)] + [weight], axis=0)
        corner = jnp.where(row4 == 0, cx, jnp.where(row4 == 1, cy, cz))
        top = (corner + 1).astype(F32) - NUDGE
        rows = jnp.where((lane4 == 0) & (row4 < 3), jnp.minimum(rows, top), rows)
        pay_ref[b] = jnp.concatenate([rows, rows], axis=0)
        return first, second

    none = jnp.full((1, LANES), BLOCKS, I32)
    first, second = lax.fori_loop(0, BLOCKS, payload, (none, none))
    pay_ref[BLOCKS] = jnp.zeros((8, LANES), F32)
    home_ref[...] = jnp.where(row8 == 0, first, second)
    copy = pltpu.make_async_copy(home_ref, homes_ref, sem)
    copy.start()
    copy.wait()

    def put(i, carry):
        for u in range(4):
            d = i * 4 + u
            first = jnp.clip(homes_ref[0, d], 0, BLOCKS)
            second = jnp.clip(homes_ref[1, d], 0, BLOCKS)
            out_ref[d] = jnp.where(row8 < 4, pay_ref[first], pay_ref[second])
        return carry

    lax.fori_loop(0, BRICKS // 4, put, 0)


def pack_gauss(gcount_ref, mean_ref, opacity_ref, gauss_ref):
    lane = iota((1, LANES), 1)
    for y in range(CY):
        for q in range(QUADS):
            mean = jnp.concatenate([mean_ref[0, y, :, 4 * q + r, :] for r in range(4)], axis=1)
            opacity = jnp.concatenate(
                [opacity_ref[0, y, 4 * q + r : 4 * q + r + 1, :] for r in range(4)], axis=1
            )
            have = [gcount_ref[0, y, 4 * q + r] for r in range(4)]
            count = jnp.where(
                lane < 64,
                jnp.where(lane < 32, have[0], have[1]),
                jnp.where(lane < 96, have[2], have[3]),
            )
            opacity = jnp.where((lane & 31) < count, opacity, 0.0)
            gauss_ref[y, q] = jnp.concatenate([mean, opacity, jnp.zeros((4, LANES), F32)], axis=0)


def side(o, last):
    if o == 0:
        return 0, 1, last + 1
    return (last, 0, 1) if o > 0 else (0, last + 2, 1)


def halo_copies(gauss_ref, halo_ref, send_sem, recv_sem):
    copies = []
    for d, (ox, oy, oz) in enumerate(OFFSETS):
        sy, ty, ny = side(oy, CY - 1)
        sq, tq, nq = side(oz, QUADS - 1)
        copies.append(
            pltpu.make_async_remote_copy(
                src_ref=gauss_ref.at[pl.ds(sy, ny), pl.ds(sq, nq), pl.ds(0, 4)],
                dst_ref=halo_ref.at[1 - ox, pl.ds(ty, ny), pl.ds(tq, nq), pl.ds(0, 4)],
                send_sem=send_sem.at[d],
                recv_sem=recv_sem.at[d],
                device_id=neighbour((ox, oy, oz)),
                device_id_type=MESH,
            )
        )
    return copies


def near_copies(part_ref, box_ref, send_sem, recv_sem):
    copies = []
    for d, (ox, oy, oz) in enumerate(OFFSETS):
        y0, ny = (1, CY) if oy == 0 else ((CY + 1, 1) if oy > 0 else (0, 1))
        copies.append(
            pltpu.make_async_remote_copy(
                src_ref=part_ref.at[pl.ds((1 + ox) * ROWS + y0, ny)],
                dst_ref=box_ref.at[d, pl.ds(0, ny)],
                send_sem=send_sem.at[d],
                recv_sem=recv_sem.at[d],
                device_id=neighbour((ox, oy, oz)),
                device_id_type=MESH,
            )
        )
    return copies


def pull_copies(pull_ref, box_ref, send_sem, recv_sem):
    copies = []
    for d, (ox, oy, oz) in enumerate(OFFSETS):
        y0, ny = (1, CY) if oy == 0 else ((CY + 1, 1) if oy > 0 else (0, 1))
        m0, nm = (0, 2) if oz == 0 else (2, 1)
        copies.append(
            pltpu.make_async_remote_copy(
                src_ref=pull_ref.at[pl.ds(m0, nm), pl.ds((1 + ox) * ROWS + y0, ny)],
                dst_ref=box_ref.at[d, pl.ds(0, nm), pl.ds(0, ny)],
                send_sem=send_sem.at[d],
                recv_sem=recv_sem.at[d],
                device_id=neighbour((ox, oy, oz)),
                device_id_type=MESH,
            )
        )
    return copies


def inverse_copies(inv_ref, send_sem, recv_sem):
    copies = []
    for d, (ox, oy, oz) in enumerate(OFFSETS):
        sy, ty, ny = side(oy, CY - 1)
        copies.append(
            pltpu.make_async_remote_copy(
                src_ref=inv_ref.at[1, pl.ds(ROWS + 1 + sy, ny)],
                dst_ref=inv_ref.at[1 - oz, pl.ds((1 - ox) * ROWS + ty, ny)],
                send_sem=send_sem.at[d],
                recv_sem=recv_sem.at[d],
                device_id=neighbour((ox, oy, oz)),
                device_id_type=MESH,
            )
        )
    return copies


def feature_windows(halo_ref, win_ref, origin, scale):
    gx, gy, gz = here()
    row8 = iota((8, LANES), 0)
    lane8 = iota((8, LANES), 1)

    def windows(y, carry):
        for x in range(3):
            window(x, y)
        return carry

    def window(x, y):
        xy = x * ROWS + y
        outside = ((x == 0) & (gx == 0)) | ((x == 2) & (gx == SX - 1))
        outside = outside | ((y == 0) & (gy == 0)) | ((y == CY + 1) & (gy == SY - 1))
        tiles = []
        for q in range(QUADS + 2):
            gone = outside
            if q == 0:
                gone = gone | (gz == 0)
            if q == QUADS + 1:
                gone = gone | (gz == SZ - 1)
            tile = halo_ref[x, y, q]
            opacity = jnp.where(gone, 0.0, tile)
            strength = jnp.where(opacity > 0.0, jnp.log2(jnp.maximum(opacity, 1e-30)) - SHARP, GONE)
            tiles.append(jnp.where(row8 == 3, strength, (tile - origin) * scale))
        for z in range(CZ):
            a, b = z // 4, z % 4
            if b == 0:
                tile = pltpu.roll(jnp.where(lane8 >= 96, tiles[a], tiles[a + 1]), 32, 1)
            elif b == 1:
                tile = tiles[a + 1]
            elif b == 2:
                tile = pltpu.roll(tiles[a + 1], 96, 1)
            else:
                tile = pltpu.roll(jnp.where(lane8 < 64, tiles[a + 2], tiles[a + 1]), 64, 1)
            tile = jnp.where((row8 == 3) & (lane8 >= 96), GONE, tile)
            win_ref[z, xy] = jnp.where(row8 == 2, tile - z * SCALE, tile)

    lax.fori_loop(0, ROWS, windows, 0)


def inverse_windows(inv_ref, win_ref):
    row8 = iota((8, LANES), 0)
    lane1 = iota((1, LANES), 1)

    def windows(y, carry):
        for x in range(3):
            window(x * ROWS + y)
        return carry

    def window(xy):
        own = inv_ref[1, xy]
        rows = [inv_ref[0, xy][QUADS - 1 : QUADS]] + [own[q : q + 1] for q in range(QUADS)]
        tile = jnp.concatenate(rows + [inv_ref[2, xy][0:1], jnp.zeros((2, LANES), F32)], axis=0)
        moved = [pltpu.roll(tile, 32, 1), tile, pltpu.roll(tile, 96, 1), pltpu.roll(tile, 64, 1)]
        for z in range(CZ):
            a, b = z // 4, z % 4
            row = moved[b][a + 1 : a + 2]
            if b == 0:
                row = jnp.where(lane1 < 32, moved[b][a : a + 1], row)
            elif b == 3:
                row = jnp.where(lane1 >= 64, moved[b][a + 2 : a + 3], row)
            win_ref[z, xy] = jnp.where(row8 == 4, row, win_ref[z, xy])

    lax.fori_loop(0, ROWS, windows, 0)


TRIPLES = [(x, dy, divmod(3 * (3 * x + dy), 4)) for x in range(3) for dy in range(3)]


def compose(win_ref, tile_ref):
    lane8 = iota((8, LANES), 1)

    def one(z, carry):
        for y in range(CY):
            tiles = [None] * (TILES + 1)
            for x, dy, (j, p) in TRIPLES:
                piece = win_ref[z, x * ROWS + y + dy]
                if p:
                    piece = pltpu.roll(piece, 32 * p, 1)
                    tiles[j] = jnp.where(lane8 < 32 * p, tiles[j], piece)
                else:
                    tiles[j] = piece
                tiles[j + 1] = piece
            for j in range(TILES):
                tile_ref[y * CZ + z, j] = tiles[j]
        return carry

    lax.fori_loop(0, CZ, one, 0)


def uncompose(tile_of, wide_ref, count):
    row8 = iota((8, LANES), 0)
    lane8 = iota((8, LANES), 1)

    def one(z, carry):
        wide = [None] * COLUMNS
        for y in range(CY):
            tiles = []
            for j in range(TILES):
                at = y * CZ + z
                rows = [jnp.sum(tile_of(at, j, k), axis=0, keepdims=True) for k in range(count)]
                tile = spread(rows[0])
                for k in range(1, count):
                    tile = jnp.where((row8 & 3) == k, rows[k], tile)
                tiles.append(tile)
            for x, dy, (j, p) in TRIPLES:
                tile = tiles[j]
                if p:
                    tile = pltpu.roll(jnp.where(lane8 >= 32 * p, tiles[j], tiles[j + 1]), LANES - 32 * p, 1)
                at = x * ROWS + y + dy
                wide[at] = tile if wide[at] is None else wide[at] + tile
        for at in range(COLUMNS):
            wide_ref[z, at] = jnp.where(lane8 < 96, wide[at], 0.0)
        return carry

    lax.fori_loop(0, CZ, one, 0)


def clear(ref):
    def one(c, carry):
        for j in range(ref.shape[1]):
            ref[c, j] = jnp.zeros((8, LANES), F32)
        return carry

    lax.fori_loop(0, CELLS, one, 0)


def fold_quads(wide_ref, xy, lane8):
    quads = [jnp.zeros((8, LANES), F32) for q in range(QUADS + 2)]
    for z in range(CZ):
        tile = wide_ref[z, xy]
        a, b = z // 4, z % 4
        if b == 1:
            quads[a + 1] = quads[a + 1] + tile
        elif b == 2:
            quads[a + 1] = quads[a + 1] + pltpu.roll(tile, 32, 1)
        elif b == 0:
            moved = pltpu.roll(tile, 96, 1)
            quads[a] = quads[a] + jnp.where(lane8 >= 96, moved, 0.0)
            quads[a + 1] = quads[a + 1] + jnp.where(lane8 < 96, moved, 0.0)
        else:
            moved = pltpu.roll(tile, 64, 1)
            quads[a + 1] = quads[a + 1] + jnp.where(lane8 >= 64, moved, 0.0)
            quads[a + 2] = quads[a + 2] + jnp.where(lane8 < 64, moved, 0.0)
    return quads


def decode(in_ref, meta_ref, metas_ref, sem):
    gx, gy, gz = here()
    row8 = iota((8, LANES), 0)
    lane8 = iota((8, LANES), 1)

    def gather(i, found):
        for u in range(32):
            s = i * 32 + u
            found = jnp.where(lane8 == s, jnp.broadcast_to(in_ref[s][:, 0:1], (8, LANES)), found)
        return found

    found = lax.fori_loop(0, BRICKS // 32, gather, jnp.zeros((8, LANES), F32))
    cell = iota((CELLS, LANES), 0).astype(F32)
    lane64 = iota((CELLS, LANES), 1).astype(F32)
    slot = jnp.full((CELLS, LANES), -1.0, F32)
    labels = []
    for k in range(2):
        y0 = jnp.floor(found[4 * k + 1 : 4 * k + 2]) - (gy * CY).astype(F32)
        z0 = jnp.floor(found[4 * k + 2 : 4 * k + 3]) - (gz * CZ).astype(F32)
        label = jnp.where(found[4 * k + 3 : 4 * k + 4] > 0.0, y0 * CZ + z0, -1.0)
        slot = jnp.where(label == cell, 2.0 * lane64 + k, slot)
        labels.append(jnp.clip(label, 0.0, CELLS - 1.0))
    slot = jnp.max(slot, axis=1, keepdims=True)
    meta_ref[pl.ds(0, CELLS), :] = jnp.broadcast_to(slot, (CELLS, LANES)).astype(I32)
    meta_ref[pl.ds(CELLS, 8), :] = jnp.where(row8 == 0, labels[0], labels[1]).astype(I32)
    copy = pltpu.make_async_copy(meta_ref, metas_ref, sem)
    copy.start()
    copy.wait()


def take_points(in_ref, metas_ref, pts_ref, origin, scale):
    row8 = iota((8, LANES), 0)

    def prepare(i, carry):
        for u in range(8):
            c = i * 8 + u
            slot = metas_ref[c, 0]
            safe = jnp.clip(slot, 0, 2 * BRICKS - 1)
            tile = in_ref[safe >> 1]
            tile = jnp.where((safe & 1) == 1, pltpu.roll(tile, 4, 0), tile)
            tile = jnp.where(slot >= 0, tile, 0.0)
            shift = origin + jnp.where(row8 == 2, (c % CZ).astype(F32), 0.0)
            pts_ref[c] = (tile - shift) * scale
        return carry

    lax.fori_loop(0, CELLS // 8, prepare, 0)
    pts_ref[CELLS] = jnp.zeros((8, LANES), F32)


def turn(pts_ref, feat_ref, c, f, at):
    row = jnp.broadcast_to(pts_ref[c, pl.ds(f, 1), :], (LANES, LANES))
    feat_ref[pl.ds(at, GROUPS)] = jnp.transpose(row).reshape(GROUPS, 8, LANES)


def first_pass(pts_ref, feat_ref, tile_ref, late_ref, term_a_ref, term_b_ref, ip_ref, acc_ref, dens_ref, pull_ref):
    weights = 3 * FEATURE
    for f in range(4):
        turn(pts_ref, feat_ref, 0, f, f * FEATURE)
    for g in range(PART):
        late_ref[PART + g] = jnp.zeros((8, LANES), F32)
    for k in range(TILES * PART):
        term_b_ref[k] = jnp.zeros((8, LANES), F32)

    def weight_of(c, g):
        return feat_ref[weights + c % 2 * GROUPS + g]

    def settle(c, part, term_ref, weight=None):
        weight = [weight_of(c, part * PART + g) for g in range(PART)] if weight is None else weight
        inverse = []
        for g in range(PART):
            at = part * PART + g
            total = jnp.sum(late_ref[at], axis=1, keepdims=True)
            inverse.append(1.0 / (FLOOR + jnp.broadcast_to(total, (8, LANES))))
            ip_ref[c * GROUPS + at] = jnp.where(weight[g] > 0.0, inverse[g], 1.0)
        for j in range(TILES):
            dense = dens_ref[c, j]
            for g in range(PART):
                dense = dense + term_ref[PART * j + g] * inverse[g]
            dens_ref[c, j] = dense

    def features(c, part):
        base = c * GROUPS + part * PART
        feats = [[feat_ref[f * FEATURE + base + g] for f in range(3)] for g in range(PART)]
        return feats, [weight_of(c, part * PART + g) for g in range(PART)]

    def main(c, part, term_ref, feats, weight):
        base = c * GROUPS + part * PART
        sums = [None] * PART
        for j in range(TILES):
            mx, my, mz, la = [spread(tile_ref[c, j, f : f + 1, :]) for f in range(4)]
            far = None
            for g in range(PART):
                px, py, pz = feats[g]
                ex, ey, ez = px - mx, py - my, pz - mz
                fall = jnp.exp2(LIFT - ex * ex - ey * ey - ez * ez)
                near = jnp.exp2(fall + la)
                term = near * weight[g]
                sums[g] = near if sums[g] is None else sums[g] + near
                far = term if far is None else far + term
                term_ref[PART * j + g] = term
                pull_ref[base + g, j] = term * fall
            acc_ref[c, 3 * j] = acc_ref[c, 3 * j] + far
        for g in range(PART):
            late_ref[part * PART + g] = sums[g]

    def sweep(c, carry):
        loaded = [features(c, part) for part in range(2)]
        settle((c + CELLS - 1) % CELLS, 1, term_b_ref)
        ahead = (c + 1) * GROUPS
        for f in range(3):
            turn(pts_ref, feat_ref, c + 1, f, f * FEATURE + ahead)
        turn(pts_ref, feat_ref, c + 1, 3, weights + (c + 1) % 2 * GROUPS)
        main(c, 0, term_a_ref, *loaded[0])
        settle(c, 0, term_a_ref, loaded[0][1])
        main(c, 1, term_b_ref, *loaded[1])
        return carry

    lax.fori_loop(0, CELLS, sweep, 0)
    settle(CELLS - 1, 1, term_b_ref)


def second_pass(feat_ref, tile_ref, late_ref, ip_ref, acc_ref, pull_ref):
    halves = CELLS * GROUPS // HALF
    for g in range(4 * HALF):
        late_ref[g] = jnp.ones((8, LANES), F32)
    lane = iota((8, LANES), 1) & 3

    def settle(h):
        for g in range(HALF):
            out = WIDTH * jnp.log(late_ref[4 * g + 3])
            for k in range(3):
                total = jnp.sum(late_ref[4 * g + k], axis=1, keepdims=True) * BACK
                out = jnp.where(lane == k + 1, total, out)
            ip_ref[h * HALF + g] = out

    def sweep(h, carry):
        c = h // 2
        base = h * HALF
        feats = [[feat_ref[f * FEATURE + base + g] for f in range(3)] for g in range(HALF)]
        inverse = [ip_ref[base + g] for g in range(HALF)]
        settle((h + halves) % (halves + 1))
        sums = [[None] * 3 for g in range(HALF)]
        for j in range(TILES):
            mx, my, mz, ig = [spread(tile_ref[c, j, f : f + 1, :]) for f in (0, 1, 2, 4)]
            far = [None] * 3
            for g in range(HALF):
                px, py, pz = feats[g]
                pull = pull_ref[base + g, j] * (inverse[g] + ig)
                parts = [pull * (px - mx), pull * (py - my), pull * (pz - mz)]
                sums[g] = [p if s is None else s + p for s, p in zip(sums[g], parts)]
                far = [p if s is None else s + p for s, p in zip(far, parts)]
            for k in range(3):
                acc_ref[c, 3 * j + k] = acc_ref[c, 3 * j + k] + far[k]
        for g in range(HALF):
            for k in range(3):
                late_ref[4 * g + k] = sums[g][k]
            late_ref[4 * g + 3] = inverse[g]
        return carry

    lax.fori_loop(0, halves, sweep, 0)
    settle(halves - 1)


def answer_points(ip_ref, res_ref, metas_ref, reply_ref):
    row8 = iota((8, LANES), 0)

    def turn(i, carry):
        for u in range(8):
            tall = ip_ref[pl.ds((i * 8 + u) * GROUPS, GROUPS)].reshape(LANES, LANES)
            res_ref[i * 8 + u] = jnp.transpose(tall)[0:8]
        return carry

    lax.fori_loop(0, CELLS // 8, turn, 0)

    def put(i, carry):
        for u in range(4):
            s = i * 4 + u
            first = jnp.clip(metas_ref[CELLS, s], 0, CELLS - 1)
            second = jnp.clip(metas_ref[CELLS + 1, s], 0, CELLS - 1)
            reply_ref[s] = jnp.where(row8 < 4, res_ref[first], res_ref[second])
        return carry

    lax.fori_loop(0, BRICKS // 4, put, 0)


def quads_of(tile, oz):
    if oz == 0:
        return tile[1 : QUADS + 1]
    row = iota((QUADS, LANES), 0)
    if oz > 0:
        return jnp.where(row == 0, tile[QUADS + 1 : QUADS + 2], 0.0)
    return jnp.where(row == QUADS - 1, tile[0:1], 0.0)


def owner_row(oy, k):
    return k if oy == 0 else (0 if oy > 0 else CY - 1)


def kernel(cell_ref, count_ref, gcount_ref, xyz_ref, weight_ref, mean_ref, opacity_ref,
           point_ref, grad_ref,
           pay_ref, out_ref, in_ref, home_ref, homes_ref, gauss_ref, halo_ref, win_ref, tile_ref,
           meta_ref, metas_ref, pts_ref, feat_ref, late_ref, term_a_ref, term_b_ref, ip_ref, keep_ref, acc_ref, dens_ref, wide_ref, part_ref,
           box_ref, inv_ref, loss_ref, res_ref, ans_ref, pull_ref, pulls_ref,
           local_sem, asend, arecv, bsend, brecv, near_sem):
    gx, gy, gz = here()
    me = (gx * SY + gy) * SZ + gz
    row8 = iota((8, LANES), 0)
    lane8 = iota((8, LANES), 1)
    signal_all()
    pack_gauss(gcount_ref, mean_ref, opacity_ref, gauss_ref)
    pack_points(cell_ref, count_ref, xyz_ref, weight_ref, pay_ref, out_ref, home_ref, homes_ref, local_sem.at[0])
    pl.semaphore_wait(pltpu.get_barrier_semaphore(), BRICKS - 1)
    halo = halo_copies(gauss_ref, halo_ref, near_sem.at[0], near_sem.at[1])
    for copy in halo:
        copy.start()
    exchange_start(out_ref, in_ref, asend, arecv)
    in_ref[me] = out_ref[me]
    for y in range(CY):
        for q in range(QUADS):
            halo_ref[1, y + 1, q + 1] = gauss_ref[y, q]
    origin = jnp.where(row8 == 0, gx, jnp.where(row8 == 1, gy * CY + CY // 2, gz * CZ)).astype(F32)
    origin = jnp.where(row8 < 3, origin, 0.0)
    scale = jnp.where(row8 < 3, SCALE, 1.0).astype(F32)
    for copy in halo:
        copy.wait()
    feature_windows(halo_ref, win_ref, origin, scale)
    compose(win_ref, tile_ref)
    clear(acc_ref)
    clear(dens_ref)
    exchange_wait(out_ref, in_ref, asend, arecv)
    decode(in_ref, meta_ref, metas_ref, local_sem.at[1])
    take_points(in_ref, metas_ref, pts_ref, origin, scale)

    first_pass(pts_ref, feat_ref, tile_ref, late_ref, term_a_ref, term_b_ref, ip_ref, acc_ref, dens_ref, keep_ref)
    uncompose(lambda c, j, k: acc_ref[c, 3 * j], wide_ref, 1)

    def fold(y, carry):
        for x in range(3):
            quads = fold_quads(wide_ref, x * ROWS + y, lane8)
            rows = [quad[0:1] for quad in quads] + [jnp.zeros((2, LANES), F32)]
            part_ref[x * ROWS + y] = jnp.concatenate(rows, axis=0)
        return carry

    lax.fori_loop(0, ROWS, fold, 0)
    copies = near_copies(part_ref, box_ref, near_sem.at[2], near_sem.at[3])
    for copy in copies:
        copy.start()
    clear(acc_ref)
    sums = [part_ref[ROWS + y + 1][1 : QUADS + 1] for y in range(CY)]
    for d, (ox, oy, oz) in enumerate(OFFSETS):
        copies[d].wait_recv()
        for k in range(CY if oy == 0 else 1):
            y = owner_row(oy, k)
            sums[y] = sums[y] + quads_of(box_ref[d, k], oz)
    for y in range(CY):
        opacity = jnp.concatenate([gauss_ref[y, q][3:4] for q in range(QUADS)], axis=0)
        valid = opacity > 0.0
        total_g = FLOOR + jnp.where(valid, sums[y] / jnp.where(valid, opacity, 1.0), 0.0)
        blank = jnp.zeros((8 - QUADS, LANES), F32)
        inv_ref[1, ROWS + y + 1] = jnp.concatenate([1.0 / total_g, blank], axis=0)
        loss = jnp.where(valid, -WIDTH * jnp.log(total_g), 0.0)
        loss_ref[y] = jnp.concatenate([loss, opacity], axis=0)
    back = inverse_copies(inv_ref, near_sem.at[4], near_sem.at[5])
    for copy in back:
        copy.start()
    for copy in copies:
        copy.wait_send()
    for copy in back:
        copy.wait()
    inverse_windows(inv_ref, win_ref)
    compose(win_ref, tile_ref)

    second_pass(feat_ref, tile_ref, late_ref, ip_ref, acc_ref, keep_ref)
    reply_ref = out_ref
    answer_points(ip_ref, res_ref, metas_ref, reply_ref)
    exchange_start(reply_ref, ans_ref, bsend, brecv)
    ans_ref[me] = reply_ref[me]
    uncompose(lambda c, j, k: acc_ref[c, 3 * j + k] if k < 3 else dens_ref[c, j], wide_ref, 4)

    def fold_pull(y, carry):
        for x in range(3):
            quads = fold_quads(wide_ref, x * ROWS + y, lane8)
            for m, (low, high) in enumerate(((1, 2), (3, 4), (0, 5))):
                pull_ref[m, x * ROWS + y] = jnp.where(row8 < 4, quads[low], quads[high])
        return carry

    lax.fori_loop(0, ROWS, fold_pull, 0)
    copies = pull_copies(pull_ref, pulls_ref, near_sem.at[6], near_sem.at[7])
    for copy in copies:
        copy.start()
    sums = [[pull_ref[m, ROWS + y + 1] for m in range(2)] for y in range(CY)]
    for d, (ox, oy, oz) in enumerate(OFFSETS):
        copies[d].wait_recv()
        for k in range(CY if oy == 0 else 1):
            y = owner_row(oy, k)
            if oz == 0:
                for m in range(2):
                    sums[y][m] = sums[y][m] + pulls_ref[d, m, k]
            elif oz > 0:
                outer = pltpu.roll(pulls_ref[d, 0, k], 4, 0)
                sums[y][0] = sums[y][0] + jnp.where(row8 < 4, outer, 0.0)
            else:
                outer = pltpu.roll(pulls_ref[d, 0, k], 4, 0)
                sums[y][1] = sums[y][1] + jnp.where(row8 >= 4, outer, 0.0)
    for y in range(CY):
        for q in range(QUADS):
            m, half = divmod(q, 2)
            tile = sums[y][m][4 * half : 4 * half + 4]
            loss = loss_ref[y][q : q + 1]
            opacity = loss_ref[y][QUADS + q : QUADS + q + 1]
            valid = opacity > 0.0
            dense = loss - WIDTH * (tile / jnp.where(valid, opacity, 1.0))
            tile = jnp.where(iota((4, LANES), 0) < 3, tile * (-BACK), dense)
            tile = jnp.where(valid, tile, 0.0)
            parts = [tile[:, SLOTS * r : SLOTS * r + SLOTS] for r in range(4)]
            for r in (0, 2):
                both = jnp.concatenate(parts[r : r + 2], axis=0)
                grad_ref[pl.ds(4 * (y * CZ + 4 * q + r), 8), :] = both
    for copy in copies:
        copy.wait_send()
    exchange_wait(reply_ref, ans_ref, bsend, brecv)

    def place(i, carry):
        for u in range(4):
            tiles = []
            for k in range(2):
                b = i * 8 + u * 2 + k
                cell = cell_ref[b]
                brick = ((cell >> 10 & 7) * SY + (cell >> 8 & 3)) * SZ + (cell >> 4 & 3)
                tile = ans_ref[brick]
                half = (homes_ref[0, brick] != b).astype(I32)
                tiles.append(jnp.where(half == k, tile, pltpu.roll(tile, 4, 0)))
            point_ref[pl.ds(pl.multiple_of(i * 32 + u * 8, 8), 8), :] = jnp.where(row8 < 4, tiles[0], tiles[1])
        return carry

    lax.fori_loop(0, BLOCKS // 8, place, 0)


def on_device(point_xyz, point_weight, block_cell, block_count, gauss_mean, gauss_opacity, gauss_count):
    dma = pltpu.SemaphoreType.DMA
    point_out, gauss_grad = pl.pallas_call(
        kernel,
        out_shape=(
            jax.ShapeDtypeStruct((BLOCKS * 4, LANES), F32),
            jax.ShapeDtypeStruct((CELLS * 4, SLOTS), F32),
        ),
        in_specs=[SMEM, SMEM, SMEM, VMEM, VMEM, VMEM, VMEM],
        out_specs=(VMEM, VMEM),
        scratch_shapes=[
            pltpu.VMEM((BLOCKS + 1, 8, LANES), F32),
            pltpu.VMEM((BRICKS, 8, LANES), F32),
            pltpu.VMEM((BRICKS, 8, LANES), F32),
            pltpu.VMEM((8, LANES), I32),
            pltpu.SMEM((8, LANES), I32),
            pltpu.VMEM((CY, QUADS, 8, LANES), F32),
            pltpu.VMEM((3, ROWS, QUADS + 2, 8, LANES), F32),
            pltpu.VMEM((CZ, COLUMNS, 8, LANES), F32),
            pltpu.VMEM((CELLS, TILES, 8, LANES), F32),
            pltpu.VMEM((CELLS + 8, LANES), I32),
            pltpu.SMEM((CELLS + 8, LANES), I32),
            pltpu.VMEM((CELLS + 1, 8, LANES), F32),
            pltpu.VMEM((3 * FEATURE + 2 * GROUPS, 8, LANES), F32),
            pltpu.VMEM((4 * HALF, 8, LANES), F32),
            pltpu.VMEM((TILES * PART, 8, LANES), F32),
            pltpu.VMEM((TILES * PART, 8, LANES), F32),
            pltpu.VMEM((CELLS * GROUPS + HALF, 8, LANES), F32),
            pltpu.VMEM((CELLS * GROUPS, TILES, 8, LANES), F32),
            pltpu.VMEM((CELLS, 3 * TILES, 8, LANES), F32),
            pltpu.VMEM((CELLS, TILES, 8, LANES), F32),
            pltpu.VMEM((CZ, COLUMNS, 8, LANES), F32),
            pltpu.VMEM((COLUMNS, 8, LANES), F32),
            pltpu.VMEM((26, CY, 8, LANES), F32),
            pltpu.VMEM((3, COLUMNS, 8, LANES), F32),
            pltpu.VMEM((CY, 8, LANES), F32),
            pltpu.VMEM((CELLS, 8, LANES), F32),
            pltpu.VMEM((BRICKS, 8, LANES), F32),
            pltpu.VMEM((3, COLUMNS, 8, LANES), F32),
            pltpu.VMEM((26, 2, CY, 8, LANES), F32),
            dma((2,)),
            dma((BRICKS,)),
            dma((BRICKS,)),
            dma((BRICKS,)),
            dma((BRICKS,)),
            dma((8, 26)),
        ],
        compiler_params=pltpu.CompilerParams(
            collective_id=0, has_side_effects=True, vmem_limit_bytes=67043328
        ),
        name="chamfer",
    )(
        block_cell,
        block_count,
        gauss_count,
        point_xyz.transpose(1, 0, 2),
        point_weight,
        gauss_mean.transpose(0, 1, 3, 2, 4),
        gauss_opacity,
    )
    return point_out.reshape(BLOCKS, 4, LANES), gauss_grad.reshape(1, CY, CZ, 4, SLOTS)


def solution(mesh):
    return jax.shard_map(
        on_device,
        mesh=mesh,
        in_specs=(
            P(AXES, None, None),
            P(AXES, None),
            P(AXES),
            P(AXES),
            P("gx", "gy", "gz", None, None),
            P("gx", "gy", "gz", None),
            P("gx", "gy", "gz"),
        ),
        out_specs=(P(AXES, None, None), P("gx", "gy", "gz", None, None)),
        check_vma=False,
    )
```
